32 devices in a mesh: fields: 2 (over x), col: 4 (over z), row: 4 (over y, core).
Axes of the slice: x: 2, y: 2, z: 4, core: 2. Of those that a mesh axis runs over, the one named last changes fastest.
Arguments:
- field_u: bfloat16 [64, 128, 128, 128], P('fields', None, 'row', 'col'), parts along dimension 0
- fac_a: bfloat16 [256, 128], P('fields'), parts along dimension 0
- fac_b: bfloat16 [256, 128], P('fields'), parts along dimension 0
- fac_c: bfloat16 [256, 128], P('fields'), parts along dimension 0
- diag_d: float32 [256, 128, 128], P(('fields', 'row'), 'col'), parts along dimension 0
Outputs:
- output: float32 [64, 128, 128, 128], P('fields', None, 'row', 'col'), parts along dimension 0
There are 2 independent parts. The reference program is written for one: setup_inputs(seed, part) draws one part's arguments, and reference() takes and returns one part's arrays. A program takes and returns all parts, laid end to end along the dimension named above; each array names one.
All inputs are finite; a program needn't handle non-finite values.
Results may differ from the reference program's by a relative error of at most 0.001.
Values are sent between devices in bfloat16 or wider.
A program may use at most 1 GiB of HBM per device.

```python
import jax
import jax.numpy as jnp
from jax import lax

N = 128
BATCH = 32


def setup_inputs(seed: int = 0, part: int = 0) -> dict:
    base_key = jax.random.fold_in(jax.random.key(seed), part)
    key_field, key_a, key_b, key_c, key_diag = jax.random.split(base_key, 5)
    fan_scale = N ** -0.5
    field_u = jax.random.normal(key_field, (BATCH, N, N, N), jnp.float32)
    fac_a = jax.random.normal(key_a, (N, N), jnp.float32) * fan_scale
    fac_b = jax.random.normal(key_b, (N, N), jnp.float32) * fan_scale
    fac_c = jax.random.normal(key_c, (N, N), jnp.float32) * fan_scale
    diag_d = jnp.exp(0.5 * jax.random.normal(key_diag, (N, N, N), jnp.float32))
    return {"field_u": field_u.astype(jnp.bfloat16), "fac_a": fac_a.astype(jnp.bfloat16), "fac_b": fac_b.astype(jnp.bfloat16), "fac_c": fac_c.astype(jnp.bfloat16), "diag_d": diag_d}


def reference(field_u, fac_a, fac_b, fac_c, diag_d):
    mat_a = fac_a.astype(jnp.float32)
    mat_b = fac_b.astype(jnp.float32)
    mat_c = fac_c.astype(jnp.float32)
    scales = diag_d.astype(jnp.float32)

    def to_bf16(values_in):
        return values_in.astype(jnp.bfloat16).astype(jnp.float32)

    def one_tensor(tensor):
        stage_one = to_bf16(jnp.einsum("ix,xyz->iyz", mat_a, tensor.astype(jnp.float32)))
        stage_two = to_bf16(jnp.einsum("jy,iyz->ijz", mat_b, stage_one))
        stage_three = to_bf16(jnp.einsum("kz,ijz->ijk", mat_c, stage_two) * scales)
        stage_four = to_bf16(jnp.einsum("kz,ijk->ijz", mat_c, stage_three))
        stage_five = to_bf16(jnp.einsum("jy,ijz->iyz", mat_b, stage_four))
        return jnp.einsum("ix,iyz->xyz", mat_a, stage_five)

    return lax.map(one_tensor, field_u)
```

```python
import functools

import jax
import jax.numpy as jnp
from jax import lax
from jax.experimental import pallas as pl
from jax.experimental.pallas import tpu as pltpu
from jax.sharding import PartitionSpec as P

MESH = pl.DeviceIdType.MESH
N = 128
S = 32
PITCH = 136
GROUP = 4
F32, BF16 = jnp.float32, jnp.bfloat16

ORDER = [
    (0, 2), (2, 3), (1, 3), (3, 2), (0, 1), (2, 1), (2, 0),
    (1, 2), (3, 3), (0, 3), (2, 2), (1, 1), (3, 1), (3, 0), (1, 0),
]


def xor(value, bits):
    if bits == 0:
        return value
    if bits == 1:
        return value + 1 - 2 * lax.rem(value, 2)
    if bits == 2:
        return lax.rem(value + 2, 4)
    return 3 - value


def part(index):
    return pl.ds(pl.multiple_of(index * S, S), S)


def dot(lhs, rhs, lhs_dim, rhs_dim):
    return lax.dot_general(lhs, rhs, (((lhs_dim,), (rhs_dim,)), ((), ())), preferred_element_type=F32)


def exchange_kernel(
    u_ref, a_ref, b_ref, c_ref, d_ref, o_ref,
    tensors, scales, work, results, b_t,
    go_send, go_recv, d_send, d_recv, back_send, back_recv,
):
    row, col = lax.axis_index("row"), lax.axis_index("col")
    me = row * 4 + col

    def device(dr, dc):
        return {"row": xor(row, dr), "col": xor(col, dc)}

    def rank(dr, dc):
        return xor(row, dr) * 4 + xor(col, dc)

    barrier = pltpu.get_barrier_semaphore()
    for dr, dc in ORDER:
        pl.semaphore_signal(barrier, inc=1, device_id=device(dr, dc), device_id_type=MESH)
    pl.semaphore_wait(barrier, len(ORDER))

    def go(t, dr, dc):
        return pltpu.make_async_remote_copy(
            src_ref=u_ref.at[t * 16 + rank(dr, dc)],
            dst_ref=tensors.at[t, part(row), part(col), :],
            send_sem=go_send.at[t, dr * 4 + dc],
            recv_sem=go_recv.at[t, dr * 4 + dc],
            device_id=device(dr, dc),
            device_id_type=MESH,
        )

    def go_own(t):
        return pltpu.make_async_copy(
            u_ref.at[t * 16 + me], tensors.at[t, part(row), part(col), :], go_recv.at[t, 0]
        )

    def spread(slot, src, dst, dr, dc):
        return pltpu.make_async_remote_copy(
            src_ref=src, dst_ref=dst, send_sem=d_send.at[slot], recv_sem=d_recv.at[slot],
            device_id=device(dr, dc), device_id_type=MESH,
        )

    def back(t, dr, dc):
        return pltpu.make_async_remote_copy(
            src_ref=results.at[t, part(xor(row, dr)), part(xor(col, dc)), :],
            dst_ref=o_ref.at[t * 16 + me],
            send_sem=back_send.at[t, dr * 4 + dc],
            recv_sem=back_recv.at[t, dr * 4 + dc],
            device_id=device(dr, dc),
            device_id_type=MESH,
        )

    def back_own(t):
        return pltpu.make_async_copy(
            results.at[t, part(row), part(col), :], o_ref.at[t * 16 + me], back_recv.at[t, 0]
        )

    own_d = scales.at[part(row), part(col), :]
    far_d = scales.at[part(row), part(xor(col, 2)), :]
    row_d = scales.at[part(row)]
    far_row_d = scales.at[part(xor(row, 2))]
    keep_d = pltpu.make_async_copy(d_ref, own_d, d_recv.at[0])
    keep_d.start()
    steps = [
        [spread(1, d_ref, own_d, 0, 2)],
        [spread(2, d_ref, own_d, 0, 1), spread(3, far_d, far_d, 0, 1)],
        [spread(4, row_d, row_d, 2, 0)],
        [spread(5, row_d, row_d, 1, 0), spread(6, far_row_d, far_row_d, 1, 0)],
    ]
    cuts = [0, 4, 8, 15, 15]
    go_own(0).start()
    for n, step in enumerate(steps):
        for copy in step:
            copy.start()
        for dr, dc in ORDER[cuts[n]:cuts[n + 1]]:
            go(0, dr, dc).start()
        if n == 1:
            keep_d.wait()
        if n < 3:
            for copy in step:
                copy.wait_recv()
    go_own(1).start()
    for dr, dc in ORDER:
        go(1, dr, dc).start()

    b_t[...] = b_ref[...].T

    def first(step, t):
        pair = tensors[t, pl.ds(step * 2, 2)].reshape(2 * N, N)
        both = dot(a_ref[...], pair, 1, 1)
        for n in range(2):
            work[pl.ds(step * 2 + n, N, stride=PITCH), :] = both[:, n * N:(n + 1) * N]

    def chain(step, t):
        del t
        rows = [pl.ds(pl.multiple_of((step * GROUP + n) * PITCH, 8), N) for n in range(GROUP)]
        h1 = jnp.concatenate([work[r, :].astype(BF16) for r in rows], axis=1)
        h2 = dot(b_ref[...], h1, 1, 0).astype(BF16)
        h2 = jnp.concatenate([h2[:, n * N:(n + 1) * N] for n in range(GROUP)], axis=0)
        h3 = dot(h2, c_ref[...], 1, 1)
        h3 = (h3 * scales[pl.ds(step * GROUP, GROUP)].reshape(GROUP * N, N)).astype(BF16)
        h4 = dot(h3, c_ref[...], 1, 0).astype(BF16)
        h4 = jnp.concatenate([h4[n * N:(n + 1) * N] for n in range(GROUP)], axis=1)
        h5 = dot(b_t[...], h4, 1, 0)
        for n in range(GROUP):
            work[rows[n], :] = h5[:, n * N:(n + 1) * N]

    def turn(step, t, base):
        for n in range(2):
            y = base + step * 2 + n
            slab = work[pl.ds(y, N, stride=PITCH), :]
            results[t, y] = slab.T.astype(BF16)

    for t in range(2):
        go_own(t).wait()
        for dr, dc in ORDER:
            go(t, dr, dc).wait_recv()
        pl.loop(0, N // 2)(functools.partial(first, t=t))
        if t == 0:
            for copy in steps[3]:
                copy.wait_recv()
        pl.loop(0, N // GROUP)(functools.partial(chain, t=t))
        for dr in (2, 3, 1, 0):
            pl.loop(0, S // 2)(functools.partial(turn, t=t, base=xor(row, dr) * S))
            for dc in (2, 3, 1, 0):
                if (dr, dc) == (0, 0):
                    back_own(t).start()
                else:
                    back(t, dr, dc).start()

    for step in steps:
        for copy in step:
            copy.wait_send()
    for t in range(2):
        back_own(t).wait()
        for dr, dc in ORDER:
            go(t, dr, dc).wait_send()
            back(t, dr, dc).wait()


def last_kernel(h_ref, a_ref, w_ref):
    w_ref[...] = dot(h_ref[...], a_ref[...], 1, 0)


def solution(mesh):
    def local_apply(field_u, fac_a, fac_b, fac_c, diag_d):
        batch = field_u.shape[0]
        any_space = pl.BlockSpec(memory_space=pl.ANY)
        vmem = pl.BlockSpec(memory_space=pltpu.VMEM)
        h5 = pl.pallas_call(
            exchange_kernel,
            out_shape=jax.ShapeDtypeStruct((batch, S, S, N), BF16),
            in_specs=[any_space, vmem, vmem, vmem, any_space],
            out_specs=any_space,
            scratch_shapes=[
                pltpu.VMEM((2, N, N, N), BF16),
                pltpu.VMEM((N, N, N), F32),
                pltpu.VMEM((N * PITCH, N), F32),
                pltpu.VMEM((2, N, N, N), BF16),
                pltpu.VMEM((N, N), BF16),
                pltpu.SemaphoreType.DMA((2, 16)),
                pltpu.SemaphoreType.DMA((2, 16)),
                pltpu.SemaphoreType.DMA((7,)),
                pltpu.SemaphoreType.DMA((7,)),
                pltpu.SemaphoreType.DMA((2, 16)),
                pltpu.SemaphoreType.DMA((2, 16)),
            ],
            compiler_params=pltpu.CompilerParams(
                collective_id=0, has_side_effects=True, vmem_limit_bytes=60 * 2**20
            ),
            name="exchange",
        )(jnp.transpose(field_u, (0, 2, 3, 1)), fac_a, fac_b, fac_c, diag_d)
        rows = batch * S * S
        block = rows // 16
        w = pl.pallas_call(
            last_kernel,
            grid=(rows // block,),
            out_shape=jax.ShapeDtypeStruct((rows, N), F32),
            in_specs=[pl.BlockSpec((block, N), lambda n: (n, 0)), pl.BlockSpec((N, N), lambda n: (0, 0))],
            out_specs=pl.BlockSpec((block, N), lambda n: (n, 0)),
            name="last",
        )(h5.reshape(rows, N), fac_a)
        return jnp.transpose(w.reshape(batch, S, S, N), (0, 3, 1, 2))

    spec_field = P("fields", None, "row", "col")
    spec_factor = P("fields", None)
    return jax.shard_map(
        local_apply,
        mesh=mesh,
        in_specs=(spec_field, spec_factor, spec_factor, spec_factor, P(("fields", "row"), "col", None)),
        out_specs=spec_field,
        check_vma=False,
    )
```

```python
import functools

import jax
import jax.numpy as jnp
from jax import lax
from jax.experimental import pallas as pl
from jax.experimental.pallas import tpu as pltpu
from jax.sharding import PartitionSpec as P

MESH = pl.DeviceIdType.MESH
N = 128
S = 32
PITCH = 136
GROUP = 4
F32, BF16 = jnp.float32, jnp.bfloat16

ORDER = [
    (0, 2), (2, 3), (1, 3), (3, 2), (0, 1), (2, 1), (2, 0),
    (1, 2), (3, 3), (0, 3), (2, 2), (1, 1), (3, 1), (3, 0), (1, 0),
]


def xor(value, bits):
    if bits == 0:
        return value
    if bits == 1:
        return value + 1 - 2 * lax.rem(value, 2)
    if bits == 2:
        return lax.rem(value + 2, 4)
    return 3 - value


def part(index):
    return pl.ds(pl.multiple_of(index * S, S), S)


def dot(lhs, rhs, lhs_dim, rhs_dim):
    return lax.dot_general(lhs, rhs, (((lhs_dim,), (rhs_dim,)), ((), ())), preferred_element_type=F32)


def exchange_kernel(
    u_ref, a_ref, b_ref, c_ref, d_ref, o_ref,
    tensors, scales, work, results, b_t,
    go_send, go_recv, d_send, d_recv, back_send, back_recv,
):
    row, col = lax.axis_index("row"), lax.axis_index("col")
    me = row * 4 + col

    def device(dr, dc):
        return {"row": xor(row, dr), "col": xor(col, dc)}

    def rank(dr, dc):
        return xor(row, dr) * 4 + xor(col, dc)

    barrier = pltpu.get_barrier_semaphore()
    for dr, dc in ORDER:
        pl.semaphore_signal(barrier, inc=1, device_id=device(dr, dc), device_id_type=MESH)
    pl.semaphore_wait(barrier, len(ORDER))

    def go(t, dr, dc):
        return pltpu.make_async_remote_copy(
            src_ref=u_ref.at[t * 16 + rank(dr, dc)],
            dst_ref=tensors.at[t, part(row), part(col), :],
            send_sem=go_send.at[t, dr * 4 + dc],
            recv_sem=go_recv.at[t, dr * 4 + dc],
            device_id=device(dr, dc),
            device_id_type=MESH,
        )

    def go_own(t):
        return pltpu.make_async_copy(
            u_ref.at[t * 16 + me], tensors.at[t, part(row), part(col), :], go_recv.at[t, 0]
        )

    def spread(slot, src, dst, dr, dc):
        return pltpu.make_async_remote_copy(
            src_ref=src, dst_ref=dst, send_sem=d_send.at[slot], recv_sem=d_recv.at[slot],
            device_id=device(dr, dc), device_id_type=MESH,
        )

    def back(t, dr, dc):
        return pltpu.make_async_remote_copy(
            src_ref=results.at[t, part(xor(row, dr)), part(xor(col, dc)), :],
            dst_ref=o_ref.at[t * 16 + me],
            send_sem=back_send.at[t, dr * 4 + dc],
            recv_sem=back_recv.at[t, dr * 4 + dc],
            device_id=device(dr, dc),
            device_id_type=MESH,
        )

    def back_own(t):
        return pltpu.make_async_copy(
            results.at[t, part(row), part(col), :], o_ref.at[t * 16 + me], back_recv.at[t, 0]
        )

    def send_back(t, dr, dc):
        if (dr, dc) == (0, 0):
            back_own(t).start()
        else:
            back(t, dr, dc).start()

    own_d = scales.at[part(row), part(col), :]
    far_d = scales.at[part(row), part(xor(col, 2)), :]
    row_d = scales.at[part(row)]
    far_row_d = scales.at[part(xor(row, 2))]
    keep_d = pltpu.make_async_copy(d_ref, own_d, d_recv.at[0])
    keep_d.start()
    steps = [
        [spread(1, d_ref, own_d, 0, 2)],
        [spread(2, d_ref, own_d, 0, 1), spread(3, far_d, far_d, 0, 1)],
        [spread(4, row_d, row_d, 2, 0)],
        [spread(5, row_d, row_d, 1, 0), spread(6, far_row_d, far_row_d, 1, 0)],
    ]
    sends = [(t, dr, dc) for t in range(2) for dr, dc in ORDER]
    cuts = [0, 4, 8, 23, 30]
    go_own(0).start()
    go_own(1).start()
    for n, step in enumerate(steps):
        for copy in step:
            copy.start()
        for t, dr, dc in sends[cuts[n]:cuts[n + 1]]:
            go(t, dr, dc).start()
        if n == 1:
            keep_d.wait()
        if n < 3:
            for copy in step:
                copy.wait_recv()

    b_t[...] = b_ref[...].T

    def first(step, t):
        pair = tensors[t, pl.ds(step * 2, 2)].reshape(2 * N, N)
        both = dot(a_ref[...], pair, 1, 1)
        for n in range(2):
            work[pl.ds(step * 2 + n, N, stride=PITCH), :] = both[:, n * N:(n + 1) * N]

    def chain(step, t):
        del t
        rows = [pl.ds(pl.multiple_of((step * GROUP + n) * PITCH, 8), N) for n in range(GROUP)]
        h1 = jnp.concatenate([work[r, :].astype(BF16) for r in rows], axis=1)
        h2 = dot(b_ref[...], h1, 1, 0).astype(BF16)
        h2 = jnp.concatenate([h2[:, n * N:(n + 1) * N] for n in range(GROUP)], axis=0)
        h3 = dot(h2, c_ref[...], 1, 1)
        h3 = (h3 * scales[pl.ds(step * GROUP, GROUP)].reshape(GROUP * N, N)).astype(BF16)
        h4 = dot(h3, c_ref[...], 1, 0).astype(BF16)
        h4 = jnp.concatenate([h4[n * N:(n + 1) * N] for n in range(GROUP)], axis=1)
        h5 = dot(b_t[...], h4, 1, 0)
        for n in range(GROUP):
            work[rows[n], :] = h5[:, n * N:(n + 1) * N]

    def turn(step, t, base):
        for n in range(2):
            y = base + step * 2 + n
            slab = work[pl.ds(y, N, stride=PITCH), :]
            results[t, y] = slab.T.astype(BF16)

    for t in range(2):
        go_own(t).wait()
        for dr, dc in ORDER:
            go(t, dr, dc).wait_recv()
        pl.loop(0, N // 2)(functools.partial(first, t=t))
        if t == 0:
            for copy in steps[3]:
                copy.wait_recv()
        pl.loop(0, N // GROUP)(functools.partial(chain, t=t))
        for dr in (2, 3, 1, 0):
            pl.loop(0, S // 2)(functools.partial(turn, t=t, base=xor(row, dr) * S))
            if t == 0:
                for dc in (2, 3, 1, 0):
                    send_back(t, dr, dc)
    for dc in (1, 0, 2, 3):
        for dr in (2, 3, 1, 0):
            send_back(1, dr, dc)

    for step in steps:
        for copy in step:
            copy.wait_send()
    for t in range(2):
        back_own(t).wait()
        for dr, dc in ORDER:
            go(t, dr, dc).wait_send()
            back(t, dr, dc).wait()


def last_kernel(h_ref, a_ref, w_ref):
    rows = w_ref.shape[0]
    start = pl.multiple_of(pl.program_id(0) * rows, rows)
    w_ref[...] = dot(h_ref[pl.ds(start, rows), :], a_ref[...], 1, 0)


def solution(mesh):
    def local_apply(field_u, fac_a, fac_b, fac_c, diag_d):
        batch = field_u.shape[0]
        any_space = pl.BlockSpec(memory_space=pl.ANY)
        vmem = pl.BlockSpec(memory_space=pltpu.VMEM)
        h5 = pl.pallas_call(
            exchange_kernel,
            out_shape=jax.ShapeDtypeStruct((batch, S, S, N), BF16),
            in_specs=[any_space, vmem, vmem, vmem, any_space],
            out_specs=any_space,
            scratch_shapes=[
                pltpu.VMEM((2, N, N, N), BF16),
                pltpu.VMEM((N, N, N), F32),
                pltpu.VMEM((N * PITCH, N), F32),
                pltpu.VMEM((2, N, N, N), BF16),
                pltpu.VMEM((N, N), BF16),
                pltpu.SemaphoreType.DMA((2, 16)),
                pltpu.SemaphoreType.DMA((2, 16)),
                pltpu.SemaphoreType.DMA((7,)),
                pltpu.SemaphoreType.DMA((7,)),
                pltpu.SemaphoreType.DMA((2, 16)),
                pltpu.SemaphoreType.DMA((2, 16)),
            ],
            compiler_params=pltpu.CompilerParams(
                collective_id=0, has_side_effects=True, vmem_limit_bytes=44 * 2**20
            ),
            name="exchange",
        )(jnp.transpose(field_u, (0, 2, 3, 1)), fac_a, fac_b, fac_c, diag_d)
        rows = batch * S * S
        block = rows // 16
        w = pl.pallas_call(
            last_kernel,
            grid=(rows // block,),
            out_shape=jax.ShapeDtypeStruct((rows, N), F32),
            in_specs=[vmem, vmem],
            out_specs=pl.BlockSpec((block, N), lambda n: (n, 0)),
            compiler_params=pltpu.CompilerParams(vmem_limit_bytes=24 * 2**20),
            name="last",
        )(h5.reshape(rows, N), fac_a)
        return jnp.transpose(w.reshape(batch, S, S, N), (0, 3, 1, 2))

    spec_field = P("fields", None, "row", "col")
    spec_factor = P("fields", None)
    return jax.shard_map(
        local_apply,
        mesh=mesh,
        in_specs=(spec_field, spec_factor, spec_factor, spec_factor, P(("fields", "row"), "col", None)),
        out_specs=spec_field,
        check_vma=False,
    )
```

```python
import functools

import jax
import jax.numpy as jnp
from jax import lax
from jax.experimental import pallas as pl
from jax.experimental.pallas import tpu as pltpu
from jax.sharding import PartitionSpec as P

MESH = pl.DeviceIdType.MESH
N = 128
S = 32
PITCH = 136
GROUP = 4
BLOCKS, BLOCK = 32, 1024
F32, BF16 = jnp.float32, jnp.bfloat16

ORDER = [
    (0, 2), (2, 3), (1, 3), (3, 2), (0, 1), (2, 1), (2, 0),
    (1, 2), (3, 3), (0, 3), (2, 2), (1, 1), (3, 1), (3, 0), (1, 0),
]


def xor(value, bits):
    if bits == 0:
        return value
    if bits == 1:
        return value + 1 - 2 * lax.rem(value, 2)
    if bits == 2:
        return lax.rem(value + 2, 4)
    return 3 - value


def part(index):
    return pl.ds(pl.multiple_of(index * S, S), S)


def dot(lhs, rhs, lhs_dim, rhs_dim):
    return lax.dot_general(lhs, rhs, (((lhs_dim,), (rhs_dim,)), ((), ())), preferred_element_type=F32)


def exchange_kernel(
    u_ref, a_hbm, b_hbm, c_hbm, d_ref, o_ref, a_out,
    tensors, scales, work, results, a_ref, b_ref, c_ref, b_t, factor_sem,
    go_send, go_recv, d_send, d_recv, back_send, back_recv,
):
    row, col = lax.axis_index("row"), lax.axis_index("col")
    me = row * 4 + col

    def device(dr, dc):
        return {"row": xor(row, dr), "col": xor(col, dc)}

    def rank(dr, dc):
        return xor(row, dr) * 4 + xor(col, dc)

    factors = [
        pltpu.make_async_copy(a_hbm, a_ref, factor_sem.at[0]),
        pltpu.make_async_copy(b_hbm, b_ref, factor_sem.at[1]),
        pltpu.make_async_copy(c_hbm, c_ref, factor_sem.at[2]),
        pltpu.make_async_copy(a_hbm, a_out, factor_sem.at[3]),
    ]
    barrier = pltpu.get_barrier_semaphore()
    for dr, dc in ORDER:
        pl.semaphore_signal(barrier, inc=1, device_id=device(dr, dc), device_id_type=MESH)
    pl.semaphore_wait(barrier, len(ORDER))

    def go(t, dr, dc):
        return pltpu.make_async_remote_copy(
            src_ref=u_ref.at[t * 16 + rank(dr, dc)],
            dst_ref=tensors.at[t, part(row), part(col), :],
            send_sem=go_send.at[t, dr * 4 + dc],
            recv_sem=go_recv.at[t, dr * 4 + dc],
            device_id=device(dr, dc),
            device_id_type=MESH,
        )

    def go_own(t):
        return pltpu.make_async_copy(
            u_ref.at[t * 16 + me], tensors.at[t, part(row), part(col), :], go_recv.at[t, 0]
        )

    def spread(slot, src, dst, dr, dc):
        return pltpu.make_async_remote_copy(
            src_ref=src, dst_ref=dst, send_sem=d_send.at[slot], recv_sem=d_recv.at[slot],
            device_id=device(dr, dc), device_id_type=MESH,
        )

    def back(t, dr, dc):
        return pltpu.make_async_remote_copy(
            src_ref=results.at[t, part(xor(row, dr)), part(xor(col, dc)), :],
            dst_ref=o_ref.at[t * 16 + me],
            send_sem=back_send.at[t, dr * 4 + dc],
            recv_sem=back_recv.at[t, dr * 4 + dc],
            device_id=device(dr, dc),
            device_id_type=MESH,
        )

    def back_own(t):
        return pltpu.make_async_copy(
            results.at[t, part(row), part(col), :], o_ref.at[t * 16 + me], back_recv.at[t, 0]
        )

    def send_back(t, dr, dc):
        if (dr, dc) == (0, 0):
            back_own(t).start()
        else:
            back(t, dr, dc).start()

    own_d = scales.at[part(row), part(col), :]
    far_d = scales.at[part(row), part(xor(col, 2)), :]
    row_d = scales.at[part(row)]
    far_row_d = scales.at[part(xor(row, 2))]
    keep_d = pltpu.make_async_copy(d_ref, own_d, d_recv.at[0])
    keep_d.start()
    steps = [
        [spread(1, d_ref, own_d, 0, 2)],
        [spread(2, d_ref, own_d, 0, 1), spread(3, far_d, far_d, 0, 1)],
        [spread(4, row_d, row_d, 2, 0)],
        [spread(5, row_d, row_d, 1, 0), spread(6, far_row_d, far_row_d, 1, 0)],
    ]
    sends = [(t, dr, dc) for t in range(2) for dr, dc in ORDER]
    cuts = [0, 4, 8, 23, 30]
    go_own(0).start()
    go_own(1).start()
    for n, step in enumerate(steps):
        for copy in step:
            copy.start()
        for t, dr, dc in sends[cuts[n]:cuts[n + 1]]:
            go(t, dr, dc).start()
        if n == 1:
            keep_d.wait()
        if n < 3:
            for copy in step:
                copy.wait_recv()

    for copy in factors:
        copy.start()
    for copy in factors:
        copy.wait()
    b_t[...] = b_ref[...].T

    def first(step, t):
        pair = tensors[t, pl.ds(step * 2, 2)].reshape(2 * N, N)
        both = dot(a_ref[...], pair, 1, 1)
        for n in range(2):
            work[pl.ds(step * 2 + n, N, stride=PITCH), :] = both[:, n * N:(n + 1) * N]

    def chain(step, t):
        del t
        rows = [pl.ds(pl.multiple_of((step * GROUP + n) * PITCH, 8), N) for n in range(GROUP)]
        h1 = jnp.concatenate([work[r, :].astype(BF16) for r in rows], axis=1)
        h2 = dot(b_ref[...], h1, 1, 0).astype(BF16)
        h2 = jnp.concatenate([h2[:, n * N:(n + 1) * N] for n in range(GROUP)], axis=0)
        h3 = dot(h2, c_ref[...], 1, 1)
        h3 = (h3 * scales[pl.ds(step * GROUP, GROUP)].reshape(GROUP * N, N)).astype(BF16)
        h4 = dot(h3, c_ref[...], 1, 0).astype(BF16)
        h4 = jnp.concatenate([h4[n * N:(n + 1) * N] for n in range(GROUP)], axis=1)
        h5 = dot(b_t[...], h4, 1, 0)
        for n in range(GROUP):
            work[rows[n], :] = h5[:, n * N:(n + 1) * N]

    def turn(step, t, base):
        for n in range(2):
            y = base + step * 2 + n
            slab = work[pl.ds(y, N, stride=PITCH), :]
            results[t, y] = slab.T.astype(BF16)

    for t in range(2):
        go_own(t).wait()
        for dr, dc in ORDER:
            go(t, dr, dc).wait_recv()
        pl.loop(0, N // 2)(functools.partial(first, t=t))
        if t == 0:
            for copy in steps[3]:
                copy.wait_recv()
        pl.loop(0, N // GROUP)(functools.partial(chain, t=t))
        for dr in (2, 3, 1, 0):
            pl.loop(0, S // 2)(functools.partial(turn, t=t, base=xor(row, dr) * S))
            if t == 0:
                for dc in (2, 3, 1, 0):
                    send_back(t, dr, dc)
    for dc in (1, 0, 2, 3):
        for dr in (2, 3, 1, 0):
            send_back(1, dr, dc)

    for step in steps:
        for copy in step:
            copy.wait_send()
    for t in range(2):
        back_own(t).wait()
        for dr, dc in ORDER:
            go(t, dr, dc).wait_send()
            back(t, dr, dc).wait()


def last_kernel(h_ref, a_ref, w_ref, out, sem):
    def store(n):
        rows = pl.ds(pl.multiple_of(n * BLOCK, BLOCK), BLOCK)
        return pltpu.make_async_copy(out.at[rows], w_ref.at[rows], sem.at[n])

    @pl.loop(0, BLOCKS)
    def _(n):
        rows = pl.ds(pl.multiple_of(n * BLOCK, BLOCK), BLOCK)
        out[rows, :] = dot(h_ref[rows, :], a_ref[...], 1, 0)
        store(n).start()

    @pl.loop(0, BLOCKS)
    def _(n):
        store(n).wait()


def solution(mesh):
    def local_apply(field_u, fac_a, fac_b, fac_c, diag_d):
        batch = field_u.shape[0]
        any_space = pl.BlockSpec(memory_space=pl.ANY)
        vmem = pl.BlockSpec(memory_space=pltpu.VMEM)

        def in_hbm(array):
            return pltpu.with_memory_space_constraint(array, pltpu.HBM)

        operands = (jnp.transpose(field_u, (0, 2, 3, 1)), fac_a, fac_b, fac_c, diag_d)
        h5, last_a = pl.pallas_call(
            exchange_kernel,
            out_shape=(pltpu.VMEM((batch, S, S, N), BF16), pltpu.VMEM((N, N), BF16)),
            in_specs=[any_space] * 5,
            out_specs=(any_space, any_space),
            scratch_shapes=[
                pltpu.VMEM((2, N, N, N), BF16),
                pltpu.VMEM((N, N, N), F32),
                pltpu.VMEM((N * PITCH, N), F32),
                pltpu.VMEM((2, N, N, N), BF16),
                pltpu.VMEM((N, N), BF16),
                pltpu.VMEM((N, N), BF16),
                pltpu.VMEM((N, N), BF16),
                pltpu.VMEM((N, N), BF16),
                pltpu.SemaphoreType.DMA((4,)),
                pltpu.SemaphoreType.DMA((2, 16)),
                pltpu.SemaphoreType.DMA((2, 16)),
                pltpu.SemaphoreType.DMA((7,)),
                pltpu.SemaphoreType.DMA((7,)),
                pltpu.SemaphoreType.DMA((2, 16)),
                pltpu.SemaphoreType.DMA((2, 16)),
            ],
            compiler_params=pltpu.CompilerParams(
                collective_id=0, has_side_effects=True, vmem_limit_bytes=44 * 2**20
            ),
            name="exchange",
        )(*(in_hbm(operand) for operand in operands))
        w = pl.pallas_call(
            last_kernel,
            out_shape=jax.ShapeDtypeStruct((BLOCKS * BLOCK, N), F32),
            in_specs=[vmem, vmem],
            out_specs=any_space,
            scratch_shapes=[pltpu.VMEM((BLOCKS * BLOCK, N), F32), pltpu.SemaphoreType.DMA((BLOCKS,))],
            compiler_params=pltpu.CompilerParams(vmem_limit_bytes=24 * 2**20),
            name="last",
        )(h5.reshape(BLOCKS * BLOCK, N), last_a)
        return jnp.transpose(w.reshape(batch, S, S, N), (0, 3, 1, 2))

    spec_field = P("fields", None, "row", "col")
    spec_factor = P("fields", None)
    return jax.shard_map(
        local_apply,
        mesh=mesh,
        in_specs=(spec_field, spec_factor, spec_factor, spec_factor, P(("fields", "row"), "col", None)),
        out_specs=spec_field,
        check_vma=False,
    )
```

```python
import functools

import jax
import jax.numpy as jnp
from jax import lax
from jax.experimental import pallas as pl
from jax.experimental.pallas import tpu as pltpu
from jax.sharding import PartitionSpec as P

MESH = pl.DeviceIdType.MESH
N = 128
S = 32
H = 16
ROUNDS = 8
UNITS = 2 * ROUNDS
GROUP = 4
BLOCKS, BLOCK = 32, 1024
F32, BF16 = jnp.float32, jnp.bfloat16
PEERS = (1, 2, 3)


def xor(value, bits):
    if bits == 0:
        return value
    if bits == 1:
        return value + 1 - 2 * lax.rem(value, 2)
    if bits == 2:
        return lax.rem(value + 2, 4)
    return 3 - value


def chunk(index, size=S):
    return pl.ds(pl.multiple_of(index * size, size), size)


def dot(lhs, rhs, lhs_dim, rhs_dim):
    return lax.dot_general(lhs, rhs, (((lhs_dim,), (rhs_dim,)), ((), ())), preferred_element_type=F32)


def exchange_kernel(
    u_ref, a_hbm, b_hbm, c_hbm, d_ref, o_ref, a_out,
    tens, cols, rets, front, rear, diag, diag_t, a_ref, b_ref, c_ref, b_t, c_t, factor_sem,
    d_send, d_recv, row_send, row_recv, go_send, go_recv, back_send, back_recv, home_send, home_recv,
):
    row, col = lax.axis_index("row"), lax.axis_index("col")

    def copy(src, dst, send, recv, peer):
        if not peer:
            return pltpu.make_async_copy(src, dst, recv)
        return pltpu.make_async_remote_copy(
            src_ref=src, dst_ref=dst, send_sem=send, recv_sem=recv, device_id=peer, device_id_type=MESH
        )

    def row_peer(dr):
        return {"row": xor(row, dr), "col": col} if dr else None

    def col_peer(dc):
        return {"row": row, "col": xor(col, dc)} if dc else None

    def halves(unit):
        return lax.div(unit, 2), lax.rem(unit, 2)

    def row_copy(unit, dr):
        t, z = halves(unit)
        return copy(
            u_ref.at[t * 4 + xor(row, dr), :, chunk(z, H), :], tens.at[unit, chunk(row)],
            row_send.at[unit, dr], row_recv.at[unit, dr], row_peer(dr),
        )

    def go_copy(unit, dc):
        t, z = halves(unit)
        return copy(
            tens.at[unit, chunk(xor(col, dc))], cols.at[t, :, chunk(col * 2 + z, H), :],
            go_send.at[unit, dc], go_recv.at[unit, dc], col_peer(dc),
        )

    def back_copy(unit, dc):
        t, z = halves(unit)
        return copy(
            cols.at[t, :, chunk(xor(col, dc) * 2 + z, H), :], rets.at[unit, chunk(col)],
            back_send.at[unit, dc], back_recv.at[unit, dc], col_peer(dc),
        )

    def home_copy(unit, dr):
        t, z = halves(unit)
        return copy(
            rets.at[unit, chunk(xor(row, dr))], o_ref.at[t * 4 + row, :, chunk(z, H), :],
            home_send.at[unit, dr], home_recv.at[unit, dr], row_peer(dr),
        )

    def start(kind, unit):
        for peer in (*PEERS, 0):
            kind(unit, peer).start()

    def arrive(kind, unit):
        kind(unit, 0).wait()
        for peer in PEERS:
            kind(unit, peer).wait_recv()

    barrier = pltpu.get_barrier_semaphore()
    for peer in PEERS:
        pl.semaphore_signal(barrier, inc=1, device_id=row_peer(peer), device_id_type=MESH)
        pl.semaphore_signal(barrier, inc=1, device_id=col_peer(peer), device_id_type=MESH)
    pl.semaphore_wait(barrier, 2 * len(PEERS))

    @pl.loop(0, 4)
    def _(unit):
        start(row_copy, unit)

    own_d, far_d = diag.at[chunk(row, S * S)], diag.at[chunk(xor(row, 2), S * S)]
    keep_d = copy(d_ref, own_d, None, d_recv.at[0], None)
    cross_d = copy(d_ref, own_d, d_send.at[1], d_recv.at[1], row_peer(2))
    near_d = copy(d_ref, own_d, d_send.at[2], d_recv.at[2], row_peer(1))
    pass_d = copy(far_d, far_d, d_send.at[3], d_recv.at[3], row_peer(1))
    for start_d in (cross_d, near_d, keep_d):
        start_d.start()

    @pl.loop(4, 8)
    def _(unit):
        start(row_copy, unit)

    factors = [
        pltpu.make_async_copy(a_hbm, a_ref, factor_sem.at[0]),
        pltpu.make_async_copy(b_hbm, b_ref, factor_sem.at[1]),
        pltpu.make_async_copy(c_hbm, c_ref, factor_sem.at[2]),
        pltpu.make_async_copy(a_hbm, a_out, factor_sem.at[3]),
    ]
    for factor in factors:
        factor.start()
    for factor in factors:
        factor.wait()
    b_t[...] = b_ref[...].T
    c_t[...] = c_ref[...].T

    def swapped(matrix):
        @pl.loop(0, H // GROUP)
        def _(step):
            lines = [pl.ds(step * GROUP + n, N, stride=H) for n in range(GROUP)]
            side = jnp.concatenate([front[line, :].astype(BF16) for line in lines], axis=1)
            both = dot(matrix[...], side, 1, 0)
            for n, line in enumerate(lines):
                rear[line, :] = both[:, n * N:(n + 1) * N]

    def rounded(buffer, unit):
        @pl.loop(0, 4)
        def _(q):
            buffer[unit, chunk(q)] = rear[chunk(q, S * H), :].reshape(S, H, N).astype(BF16)

    def first_two(unit):
        arrive(row_copy, unit)

        @pl.loop(0, 4)
        def _(q):
            front[chunk(q, S * H), :] = dot(tens[unit, chunk(q)].reshape(S * H, N), a_ref[...], 1, 1)

        swapped(b_ref)
        rounded(tens, unit)
        start(go_copy, unit)

    def middle(t):
        arrive(go_copy, 2 * t)
        arrive(go_copy, 2 * t + 1)

        @pl.loop(0, S // GROUP)
        def _(step):
            def side(buffer):
                return jnp.concatenate([buffer[step * GROUP + n] for n in range(GROUP)], axis=1)

            h3 = (dot(c_ref[...], side(cols.at[t]), 1, 0) * side(diag_t)).astype(BF16)
            h4 = dot(c_t[...], h3, 1, 0).astype(BF16)
            for n in range(GROUP):
                cols[t, step * GROUP + n] = h4[:, n * N:(n + 1) * N]

        start(back_copy, 2 * t)
        start(back_copy, 2 * t + 1)

    def fifth(unit):
        arrive(back_copy, unit)

        @pl.loop(0, 4)
        def _(q):
            front[chunk(q, S * H), :] = rets[unit, chunk(q)].reshape(S * H, N).astype(F32)

        swapped(b_t)
        rounded(rets, unit)
        start(home_copy, unit)

    pl.loop(0, 4)(first_two)
    cross_d.wait_recv()
    pass_d.start()
    keep_d.wait()
    near_d.wait_recv()
    pass_d.wait_recv()

    @pl.loop(0, S)
    def _(j):
        diag_t[j] = diag[pl.ds(j, N, stride=S), :].T

    def body(t, rows, firsts, fifths):
        middle(t)
        if rows:
            start(row_copy, 2 * t + 8)
            start(row_copy, 2 * t + 9)
        if firsts:
            pl.loop(2 * t + 4, 2 * t + 6)(first_two)
        if fifths:
            pl.loop(2 * t - 2, 2 * t)(fifth)

    pl.loop(0, 1)(functools.partial(body, rows=True, firsts=True, fifths=False))
    pl.loop(1, 4)(functools.partial(body, rows=True, firsts=True, fifths=True))
    pl.loop(4, 6)(functools.partial(body, rows=False, firsts=True, fifths=True))
    pl.loop(6, 8)(functools.partial(body, rows=False, firsts=False, fifths=True))
    pl.loop(14, 16)(fifth)

    for sent in (cross_d, near_d, pass_d):
        sent.wait_send()

    @pl.loop(0, UNITS)
    def _(unit):
        arrive(home_copy, unit)
        for kind in (row_copy, go_copy, back_copy, home_copy):
            for peer in PEERS:
                kind(unit, peer).wait_send()


def last_kernel(h_ref, a_ref, w_ref, out, sem):
    def store(n):
        rows = chunk(n, BLOCK)
        return pltpu.make_async_copy(out.at[rows], w_ref.at[rows], sem.at[n])

    @pl.loop(0, BLOCKS)
    def _(n):
        rows = chunk(n, BLOCK)
        out[rows, :] = dot(h_ref[rows, :], a_ref[...], 1, 0)
        store(n).start()

    @pl.loop(0, BLOCKS)
    def _(n):
        store(n).wait()


def solution(mesh):
    def local_apply(field_u, fac_a, fac_b, fac_c, diag_d):
        batch = field_u.shape[0]
        any_space = pl.BlockSpec(memory_space=pl.ANY)
        vmem = pl.BlockSpec(memory_space=pltpu.VMEM)

        def in_hbm(array):
            return pltpu.with_memory_space_constraint(array, pltpu.HBM)

        operands = (jnp.transpose(field_u, (0, 2, 3, 1)), fac_a, fac_b, fac_c, diag_d.reshape(S * S, N))
        pairs = pltpu.SemaphoreType.DMA((UNITS, 4))
        h5, last_a = pl.pallas_call(
            exchange_kernel,
            out_shape=(pltpu.VMEM((batch, S, S, N), BF16), pltpu.VMEM((N, N), BF16)),
            in_specs=[any_space] * 5,
            out_specs=(any_space, any_space),
            scratch_shapes=[
                pltpu.VMEM((UNITS, N, H, N), BF16),
                pltpu.VMEM((ROUNDS, S, N, N), BF16),
                pltpu.VMEM((UNITS, N, H, N), BF16),
                pltpu.VMEM((N * H, N), F32),
                pltpu.VMEM((N * H, N), F32),
                pltpu.VMEM((N * S, N), F32),
                pltpu.VMEM((S, N, N), F32),
                pltpu.VMEM((N, N), BF16),
                pltpu.VMEM((N, N), BF16),
                pltpu.VMEM((N, N), BF16),
                pltpu.VMEM((N, N), BF16),
                pltpu.VMEM((N, N), BF16),
                pltpu.SemaphoreType.DMA((4,)),
                pltpu.SemaphoreType.DMA((4,)),
                pltpu.SemaphoreType.DMA((4,)),
                pairs, pairs, pairs, pairs, pairs, pairs, pairs, pairs,
            ],
            compiler_params=pltpu.CompilerParams(
                collective_id=0, has_side_effects=True, vmem_limit_bytes=44 * 2**20
            ),
            name="exchange",
        )(*(in_hbm(operand) for operand in operands))
        w = pl.pallas_call(
            last_kernel,
            out_shape=jax.ShapeDtypeStruct((BLOCKS * BLOCK, N), F32),
            in_specs=[vmem, vmem],
            out_specs=any_space,
            scratch_shapes=[pltpu.VMEM((BLOCKS * BLOCK, N), F32), pltpu.SemaphoreType.DMA((BLOCKS,))],
            compiler_params=pltpu.CompilerParams(vmem_limit_bytes=24 * 2**20),
            name="last",
        )(h5.reshape(BLOCKS * BLOCK, N), last_a)
        return jnp.transpose(w.reshape(batch, S, S, N), (0, 3, 1, 2))

    spec_field = P("fields", None, "row", "col")
    spec_factor = P("fields", None)
    return jax.shard_map(
        local_apply,
        mesh=mesh,
        in_specs=(spec_field, spec_factor, spec_factor, spec_factor, P(("fields", "row"), "col", None)),
        out_specs=spec_field,
        check_vma=False,
    )
```

```python
import functools

import jax
import jax.numpy as jnp
from jax import lax
from jax.experimental import pallas as pl
from jax.experimental.pallas import tpu as pltpu
from jax.sharding import PartitionSpec as P

MESH = pl.DeviceIdType.MESH
N = 128
S = 32
H = 8
PER = S // H
ROUNDS = 8
UNITS = PER * ROUNDS
GROUP = 4
BLOCKS, BLOCK = 16, 2048
F32, BF16 = jnp.float32, jnp.bfloat16
PEERS = (1, 2, 3)


def xor(value, bits):
    if bits == 0:
        return value
    if bits == 1:
        return value + 1 - 2 * lax.rem(value, 2)
    if bits == 2:
        return lax.rem(value + 2, 4)
    return 3 - value


def chunk(index, size=S):
    return pl.ds(pl.multiple_of(index * size, size), size)


def dot(lhs, rhs, lhs_dim, rhs_dim):
    return lax.dot_general(lhs, rhs, (((lhs_dim,), (rhs_dim,)), ((), ())), preferred_element_type=F32)


def exchange_kernel(
    u_ref, a_hbm, b_hbm, c_hbm, d_ref, o_ref, a_out,
    tens, cols, rets, front, rear, diag, diag_t, a_ref, b_ref, c_ref, b_t, c_t, factor_sem,
    d_send, d_recv, row_send, row_recv, go_send, go_recv, back_send, back_recv, home_send, home_recv,
):
    row, col = lax.axis_index("row"), lax.axis_index("col")

    def copy(src, dst, send, recv, peer):
        if not peer:
            return pltpu.make_async_copy(src, dst, recv)
        return pltpu.make_async_remote_copy(
            src_ref=src, dst_ref=dst, send_sem=send, recv_sem=recv, device_id=peer, device_id_type=MESH
        )

    def row_peer(dr):
        return {"row": xor(row, dr), "col": col} if dr else None

    def col_peer(dc):
        return {"row": row, "col": xor(col, dc)} if dc else None

    def halves(unit):
        return lax.div(unit, PER), lax.rem(unit, PER)

    def row_copy(unit, dr):
        t, z = halves(unit)
        return copy(
            u_ref.at[t * 4 + xor(row, dr), :, chunk(z, H), :], tens.at[unit, chunk(row)],
            row_send.at[unit, dr], row_recv.at[unit, dr], row_peer(dr),
        )

    def go_copy(unit, dc):
        t, z = halves(unit)
        return copy(
            tens.at[unit, chunk(xor(col, dc))], cols.at[t, :, chunk(col * PER + z, H), :],
            go_send.at[unit, dc], go_recv.at[unit, dc], col_peer(dc),
        )

    def back_copy(unit, dc):
        t, z = halves(unit)
        return copy(
            cols.at[t, :, chunk(xor(col, dc) * PER + z, H), :], rets.at[unit, chunk(col)],
            back_send.at[unit, dc], back_recv.at[unit, dc], col_peer(dc),
        )

    def home_copy(unit, dr):
        t, z = halves(unit)
        return copy(
            rets.at[unit, chunk(xor(row, dr))], o_ref.at[t * 4 + row, :, chunk(z, H), :],
            home_send.at[unit, dr], home_recv.at[unit, dr], row_peer(dr),
        )

    def start(kind, unit):
        for peer in (0, 3, 2, 1) if kind in (row_copy, home_copy) else (1, 2, 3, 0):
            kind(unit, peer).start()

    def arrive(kind, unit):
        kind(unit, 0).wait()
        for peer in PEERS:
            kind(unit, peer).wait_recv()

    barrier = pltpu.get_barrier_semaphore()
    for peer in PEERS:
        pl.semaphore_signal(barrier, inc=1, device_id=row_peer(peer), device_id_type=MESH)
        pl.semaphore_signal(barrier, inc=1, device_id=col_peer(peer), device_id_type=MESH)
    pl.semaphore_wait(barrier, 2 * len(PEERS))

    @pl.loop(0, 2 * PER)
    def _(unit):
        start(row_copy, unit)

    own_d, far_d = diag.at[chunk(row, S * S)], diag.at[chunk(xor(row, 2), S * S)]
    keep_d = copy(d_ref, own_d, None, d_recv.at[0], None)
    cross_d = copy(d_ref, own_d, d_send.at[1], d_recv.at[1], row_peer(2))
    near_d = copy(d_ref, own_d, d_send.at[2], d_recv.at[2], row_peer(1))
    pass_d = copy(far_d, far_d, d_send.at[3], d_recv.at[3], row_peer(1))
    for start_d in (cross_d, near_d, keep_d):
        start_d.start()

    @pl.loop(2 * PER, 4 * PER)
    def _(unit):
        start(row_copy, unit)

    factors = [
        pltpu.make_async_copy(a_hbm, a_ref, factor_sem.at[0]),
        pltpu.make_async_copy(b_hbm, b_ref, factor_sem.at[1]),
        pltpu.make_async_copy(c_hbm, c_ref, factor_sem.at[2]),
        pltpu.make_async_copy(a_hbm, a_out, factor_sem.at[3]),
    ]
    for factor in factors:
        factor.start()
    for factor in factors:
        factor.wait()
    b_t[...] = b_ref[...].T
    c_t[...] = c_ref[...].T

    def swapped(matrix):
        @pl.loop(0, H // GROUP)
        def _(step):
            lines = [pl.ds(step * GROUP + n, N, stride=H) for n in range(GROUP)]
            side = jnp.concatenate([front[line, :].astype(BF16) for line in lines], axis=1)
            both = dot(matrix[...], side, 1, 0)
            for n, line in enumerate(lines):
                rear[line, :] = both[:, n * N:(n + 1) * N]

    def rounded(buffer, unit):
        @pl.loop(0, 4)
        def _(q):
            buffer[unit, chunk(q)] = rear[chunk(q, S * H), :].reshape(S, H, N).astype(BF16)

    def first_two(unit):
        arrive(row_copy, unit)

        @pl.loop(0, 4)
        def _(q):
            front[chunk(q, S * H), :] = dot(tens[unit, chunk(q)].reshape(S * H, N), a_ref[...], 1, 1)

        swapped(b_ref)
        rounded(tens, unit)
        start(go_copy, unit)

    def middle(t):
        for n in range(PER):
            arrive(go_copy, PER * t + n)

        @pl.loop(0, S // GROUP)
        def _(step):
            def side(buffer):
                return jnp.concatenate([buffer[step * GROUP + n] for n in range(GROUP)], axis=1)

            h3 = (dot(c_ref[...], side(cols.at[t]), 1, 0) * side(diag_t)).astype(BF16)
            h4 = dot(c_t[...], h3, 1, 0).astype(BF16)
            for n in range(GROUP):
                cols[t, step * GROUP + n] = h4[:, n * N:(n + 1) * N]

        for n in range(PER):
            start(back_copy, PER * t + n)

    def fifth(unit):
        arrive(back_copy, unit)

        @pl.loop(0, 4)
        def _(q):
            front[chunk(q, S * H), :] = rets[unit, chunk(q)].reshape(S * H, N).astype(F32)

        swapped(b_t)
        rounded(rets, unit)
        start(home_copy, unit)

    pl.loop(0, 2 * PER)(first_two)
    cross_d.wait_recv()
    pass_d.start()
    keep_d.wait()
    near_d.wait_recv()
    pass_d.wait_recv()

    @pl.loop(0, S)
    def _(j):
        diag_t[j] = diag[pl.ds(j, N, stride=S), :].T

    def body(t, rows, firsts, fifths):
        middle(t)
        if rows:
            for n in range(PER):
                start(row_copy, PER * (t + 4) + n)
        if firsts:
            pl.loop(PER * (t + 2), PER * (t + 3))(first_two)
        if fifths:
            pl.loop(PER * (t - 1), PER * t)(fifth)

    pl.loop(0, 1)(functools.partial(body, rows=True, firsts=True, fifths=False))
    pl.loop(1, 4)(functools.partial(body, rows=True, firsts=True, fifths=True))
    pl.loop(4, 6)(functools.partial(body, rows=False, firsts=True, fifths=True))
    pl.loop(6, 8)(functools.partial(body, rows=False, firsts=False, fifths=True))
    pl.loop(PER * 7, PER * 8)(fifth)

    for sent in (cross_d, near_d, pass_d):
        sent.wait_send()

    @pl.loop(0, UNITS)
    def _(unit):
        arrive(home_copy, unit)
        for kind in (row_copy, go_copy, back_copy, home_copy):
            for peer in PEERS:
                kind(unit, peer).wait_send()


def last_kernel(h_ref, a_ref, w_ref, out, sem):
    def store(n):
        rows = chunk(n, BLOCK)
        return pltpu.make_async_copy(out.at[rows], w_ref.at[rows], sem.at[n])

    @pl.loop(0, BLOCKS)
    def _(n):
        rows = chunk(n, BLOCK)
        out[rows, :] = dot(h_ref[rows, :], a_ref[...], 1, 0)
        store(n).start()

    @pl.loop(0, BLOCKS)
    def _(n):
        store(n).wait()


def solution(mesh):
    def local_apply(field_u, fac_a, fac_b, fac_c, diag_d):
        batch = field_u.shape[0]
        any_space = pl.BlockSpec(memory_space=pl.ANY)
        vmem = pl.BlockSpec(memory_space=pltpu.VMEM)

        def in_hbm(array):
            return pltpu.with_memory_space_constraint(array, pltpu.HBM)

        operands = (jnp.transpose(field_u, (0, 2, 3, 1)), fac_a, fac_b, fac_c, diag_d.reshape(S * S, N))
        pairs = pltpu.SemaphoreType.DMA((UNITS, 4))
        h5, last_a = pl.pallas_call(
            exchange_kernel,
            out_shape=(pltpu.VMEM((batch, S, S, N), BF16), pltpu.VMEM((N, N), BF16)),
            in_specs=[any_space] * 5,
            out_specs=(any_space, any_space),
            scratch_shapes=[
                pltpu.VMEM((UNITS, N, H, N), BF16),
                pltpu.VMEM((ROUNDS, S, N, N), BF16),
                pltpu.VMEM((UNITS, N, H, N), BF16),
                pltpu.VMEM((N * H, N), F32),
                pltpu.VMEM((N * H, N), F32),
                pltpu.VMEM((N * S, N), F32),
                pltpu.VMEM((S, N, N), F32),
                pltpu.VMEM((N, N), BF16),
                pltpu.VMEM((N, N), BF16),
                pltpu.VMEM((N, N), BF16),
                pltpu.VMEM((N, N), BF16),
                pltpu.VMEM((N, N), BF16),
                pltpu.SemaphoreType.DMA((4,)),
                pltpu.SemaphoreType.DMA((4,)),
                pltpu.SemaphoreType.DMA((4,)),
                pairs, pairs, pairs, pairs, pairs, pairs, pairs, pairs,
            ],
            compiler_params=pltpu.CompilerParams(
                collective_id=0, has_side_effects=True, vmem_limit_bytes=44 * 2**20
            ),
            name="exchange",
        )(*(in_hbm(operand) for operand in operands))
        w = pl.pallas_call(
            last_kernel,
            out_shape=jax.ShapeDtypeStruct((BLOCKS * BLOCK, N), F32),
            in_specs=[vmem, vmem],
            out_specs=any_space,
            scratch_shapes=[pltpu.VMEM((BLOCKS * BLOCK, N), F32), pltpu.SemaphoreType.DMA((BLOCKS,))],
            compiler_params=pltpu.CompilerParams(vmem_limit_bytes=24 * 2**20),
            name="last",
        )(h5.reshape(BLOCKS * BLOCK, N), last_a)
        return jnp.transpose(w.reshape(batch, S, S, N), (0, 3, 1, 2))

    spec_field = P("fields", None, "row", "col")
    spec_factor = P("fields", None)
    return jax.shard_map(
        local_apply,
        mesh=mesh,
        in_specs=(spec_field, spec_factor, spec_factor, spec_factor, P(("fields", "row"), "col", None)),
        out_specs=spec_field,
        check_vma=False,
    )
```

```python
import functools

import jax
import jax.numpy as jnp
from jax import lax
from jax.experimental import pallas as pl
from jax.experimental.pallas import tpu as pltpu
from jax.sharding import PartitionSpec as P

MESH = pl.DeviceIdType.MESH
N = 128
S = 32
H = 16
FINE = 8
PER = S // FINE
ROUNDS = 8
EARLY = 2
LATE = 1
GROUP = 4
BLOCKS, BLOCK = 8, 4096
F32, BF16 = jnp.float32, jnp.bfloat16
PEERS = (1, 2, 3)


def xor(value, bits):
    if bits == 0:
        return value
    if bits == 1:
        return value + 1 - 2 * lax.rem(value, 2)
    if bits == 2:
        return lax.rem(value + 2, 4)
    return 3 - value


def chunk(index, size=S):
    return pl.ds(pl.multiple_of(index * size, size), size)


def dot(lhs, rhs, lhs_dim, rhs_dim):
    return lax.dot_general(lhs, rhs, (((lhs_dim,), (rhs_dim,)), ((), ())), preferred_element_type=F32)


def exchange_kernel(
    u_ref, a_hbm, b_hbm, c_hbm, d_ref, o_ref, a_out,
    fine_in, tens, cols, rets, fine_out, front, rear, diag, diag_t,
    a_ref, b_ref, c_ref, b_t, c_t, factor_sem, d_send, d_recv, *sems,
):
    row, col = lax.axis_index("row"), lax.axis_index("col")

    def row_peer(dr):
        return {"row": xor(row, dr), "col": col} if dr else None

    def col_peer(dc):
        return {"row": row, "col": xor(col, dc)} if dc else None

    def copy(src, dst, send, recv, peer):
        if not peer:
            return pltpu.make_async_copy(src, dst, recv)
        return pltpu.make_async_remote_copy(
            src_ref=src, dst_ref=dst, send_sem=send, recv_sem=recv, device_id=peer, device_id_type=MESH
        )

    def paired(which, index, offset):
        return sems[2 * which].at[index, offset], sems[2 * which + 1].at[index, offset]

    def row_round(t, dr):
        src = u_ref.at[(t + EARLY) * 4 + xor(row, dr)]
        return copy(src, tens.at[t, chunk(row)], *paired(0, t, dr), row_peer(dr))

    def row_fine(unit, dr):
        t, z = lax.div(unit, PER), lax.rem(unit, PER)
        src = u_ref.at[t * 4 + xor(row, dr), :, chunk(z, FINE), :]
        return copy(src, fine_in.at[unit, chunk(row)], *paired(1, unit, dr), row_peer(dr))

    def go_round(t, dc):
        dst = cols.at[t + EARLY, :, chunk(col), :]
        return copy(tens.at[t, chunk(xor(col, dc))], dst, *paired(2, t, dc), col_peer(dc))

    def go_fine(unit, dc):
        t, z = lax.div(unit, PER), lax.rem(unit, PER)
        dst = cols.at[t, :, chunk(col * PER + z, FINE), :]
        return copy(fine_in.at[unit, chunk(xor(col, dc))], dst, *paired(3, unit, dc), col_peer(dc))

    def back_round(t, dc):
        src = cols.at[t, :, chunk(xor(col, dc)), :]
        return copy(src, rets.at[t, chunk(col)], *paired(4, t, dc), col_peer(dc))

    def back_fine(unit, dc):
        t, z = lax.div(unit, PER) + ROUNDS - LATE, lax.rem(unit, PER)
        src = cols.at[t, :, chunk(xor(col, dc) * PER + z, FINE), :]
        return copy(src, fine_out.at[unit, chunk(col)], *paired(5, unit, dc), col_peer(dc))

    def home_round(t, dr):
        dst = o_ref.at[t * 4 + row]
        return copy(rets.at[t, chunk(xor(row, dr))], dst, *paired(6, t, dr), row_peer(dr))

    def home_fine(unit, dr):
        t, z = lax.div(unit, PER) + ROUNDS - LATE, lax.rem(unit, PER)
        dst = o_ref.at[t * 4 + row, :, chunk(z, FINE), :]
        return copy(fine_out.at[unit, chunk(xor(row, dr))], dst, *paired(7, unit, dr), row_peer(dr))

    def start(kind, index):
        for peer in (0, 3, 2, 1) if kind in (row_round, row_fine, home_round, home_fine) else (1, 2, 3, 0):
            kind(index, peer).start()

    def arrive(kind, index):
        kind(index, 0).wait()
        for peer in PEERS:
            kind(index, peer).wait_recv()

    barrier = pltpu.get_barrier_semaphore()
    for peer in PEERS:
        pl.semaphore_signal(barrier, inc=1, device_id=row_peer(peer), device_id_type=MESH)
        pl.semaphore_signal(barrier, inc=1, device_id=col_peer(peer), device_id_type=MESH)
    pl.semaphore_wait(barrier, 2 * len(PEERS))

    @pl.loop(0, PER * EARLY)
    def _(unit):
        start(row_fine, unit)

    own_d, far_d = diag.at[chunk(row, S * S)], diag.at[chunk(xor(row, 2), S * S)]
    keep_d = copy(d_ref, own_d, None, d_recv.at[0], None)
    cross_d = copy(d_ref, own_d, d_send.at[1], d_recv.at[1], row_peer(2))
    near_d = copy(d_ref, own_d, d_send.at[2], d_recv.at[2], row_peer(1))
    pass_d = copy(far_d, far_d, d_send.at[3], d_recv.at[3], row_peer(1))
    for start_d in (cross_d, near_d, keep_d):
        start_d.start()

    @pl.loop(0, 2)
    def _(t):
        start(row_round, t)

    factors = [
        pltpu.make_async_copy(a_hbm, a_ref, factor_sem.at[0]),
        pltpu.make_async_copy(b_hbm, b_ref, factor_sem.at[1]),
        pltpu.make_async_copy(c_hbm, c_ref, factor_sem.at[2]),
        pltpu.make_async_copy(a_hbm, a_out, factor_sem.at[3]),
    ]
    for factor in factors:
        factor.start()
    for factor in factors:
        factor.wait()
    b_t[...] = b_ref[...].T
    c_t[...] = c_ref[...].T

    def swapped(matrix, height):
        @pl.loop(0, height // GROUP)
        def _(step):
            lines = [pl.ds(step * GROUP + n, N, stride=height) for n in range(GROUP)]
            side = jnp.concatenate([front[line, :].astype(BF16) for line in lines], axis=1)
            both = dot(matrix[...], side, 1, 0)
            for n, line in enumerate(lines):
                rear[line, :] = both[:, n * N:(n + 1) * N]

    def first_two(view, height):
        @pl.loop(0, 4)
        def _(q):
            block = view[chunk(q)].reshape(S * height, N)
            front[chunk(q, S * height), :] = dot(block, a_ref[...], 1, 1)

        swapped(b_ref, height)

    def fifth(view, height):
        @pl.loop(0, 4)
        def _(q):
            front[chunk(q, S * height), :] = view[chunk(q)].reshape(S * height, N).astype(F32)

        swapped(b_t, height)

    def rounded(view, height):
        @pl.loop(0, 4)
        def _(q):
            view[chunk(q)] = rear[chunk(q, S * height), :].reshape(S, height, N).astype(BF16)

    def fine(here, there, buffer, work, unit):
        arrive(here, unit)
        work(buffer.at[unit], FINE)
        rounded(buffer.at[unit], FINE)
        start(there, unit)

    def whole(here, there, buffer, work, t):
        arrive(here, t)

        @pl.loop(0, S // H)
        def _(half):
            view = buffer.at[t, :, chunk(half, H), :]
            work(view, H)
            rounded(view, H)

        start(there, t)

    def middle(t, early, late):
        if early:
            for n in range(PER):
                arrive(go_fine, PER * t + n)
        else:
            arrive(go_round, t - EARLY)

        @pl.loop(0, S // GROUP)
        def _(step):
            def side(buffer):
                return jnp.concatenate([buffer[step * GROUP + n] for n in range(GROUP)], axis=1)

            h3 = (dot(c_ref[...], side(cols.at[t]), 1, 0) * side(diag_t)).astype(BF16)
            h4 = dot(c_t[...], h3, 1, 0).astype(BF16)
            for n in range(GROUP):
                cols[t, step * GROUP + n] = h4[:, n * N:(n + 1) * N]

        if late:
            for n in range(PER):
                start(back_fine, PER * (t - ROUNDS + LATE) + n)
        else:
            start(back_round, t)

    pl.loop(0, PER * EARLY)(functools.partial(fine, row_fine, go_fine, fine_in, first_two))
    cross_d.wait_recv()
    pass_d.start()
    keep_d.wait()
    near_d.wait_recv()
    pass_d.wait_recv()

    @pl.loop(0, S)
    def _(j):
        diag_t[j] = diag[pl.ds(j, N, stride=S), :].T

    def body(t, early=False, late=False, rows=False, firsts=False, fifths=True):
        middle(t, early, late)
        if rows:
            start(row_round, t + 4 - EARLY)
        if firsts:
            whole(row_round, go_round, tens, first_two, t + 2 - EARLY)
        if fifths:
            whole(back_round, home_round, rets, fifth, t - 1)

    pl.loop(0, 1)(functools.partial(body, early=True, rows=True, firsts=True, fifths=False))
    pl.loop(1, 2)(functools.partial(body, early=True, rows=True, firsts=True))
    pl.loop(2, 4)(functools.partial(body, rows=True, firsts=True))
    pl.loop(4, 6)(functools.partial(body, firsts=True))
    pl.loop(6, 7)(body)
    pl.loop(7, 8)(functools.partial(body, late=True))
    pl.loop(0, PER * LATE)(functools.partial(fine, back_fine, home_fine, fine_out, fifth))

    def finish(kinds, index):
        for kind in kinds:
            if kind in (home_round, home_fine):
                arrive(kind, index)
            for peer in PEERS:
                kind(index, peer).wait_send()

    for sent in (cross_d, near_d, pass_d):
        sent.wait_send()
    pl.loop(0, PER * EARLY)(functools.partial(finish, (row_fine, go_fine)))
    pl.loop(0, ROUNDS - EARLY)(functools.partial(finish, (row_round, go_round)))
    pl.loop(0, ROUNDS - LATE)(functools.partial(finish, (back_round, home_round)))
    pl.loop(0, PER * LATE)(functools.partial(finish, (back_fine, home_fine)))


def last_kernel(h_ref, a_ref, w_ref, out, sem):
    def store(n):
        rows = chunk(n, BLOCK)
        return pltpu.make_async_copy(out.at[rows], w_ref.at[rows], sem.at[n])

    @pl.loop(0, BLOCKS)
    def _(n):
        rows = chunk(n, BLOCK)
        out[rows, :] = dot(h_ref[rows, :], a_ref[...], 1, 0)
        store(n).start()

    @pl.loop(0, BLOCKS)
    def _(n):
        store(n).wait()


def solution(mesh):
    def local_apply(field_u, fac_a, fac_b, fac_c, diag_d):
        batch = field_u.shape[0]
        any_space = pl.BlockSpec(memory_space=pl.ANY)
        vmem = pl.BlockSpec(memory_space=pltpu.VMEM)

        def in_hbm(array):
            return pltpu.with_memory_space_constraint(array, pltpu.HBM)

        operands = (jnp.transpose(field_u, (0, 2, 3, 1)), fac_a, fac_b, fac_c, diag_d.reshape(S * S, N))
        counts = (ROUNDS - EARLY, PER * EARLY) * 2 + (ROUNDS - LATE, PER * LATE) * 2
        pairs = [pltpu.SemaphoreType.DMA((n, 4)) for n in counts for _ in range(2)]
        h5, last_a = pl.pallas_call(
            exchange_kernel,
            out_shape=(pltpu.VMEM((batch, S, S, N), BF16), pltpu.VMEM((N, N), BF16)),
            in_specs=[any_space] * 5,
            out_specs=(any_space, any_space),
            scratch_shapes=[
                pltpu.VMEM((PER * EARLY, N, FINE, N), BF16),
                pltpu.VMEM((ROUNDS - EARLY, N, S, N), BF16),
                pltpu.VMEM((ROUNDS, S, N, N), BF16),
                pltpu.VMEM((ROUNDS - LATE, N, S, N), BF16),
                pltpu.VMEM((PER * LATE, N, FINE, N), BF16),
                pltpu.VMEM((N * H, N), F32),
                pltpu.VMEM((N * H, N), F32),
                pltpu.VMEM((N * S, N), F32),
                pltpu.VMEM((S, N, N), F32),
                pltpu.VMEM((N, N), BF16),
                pltpu.VMEM((N, N), BF16),
                pltpu.VMEM((N, N), BF16),
                pltpu.VMEM((N, N), BF16),
                pltpu.VMEM((N, N), BF16),
                pltpu.SemaphoreType.DMA((4,)),
                pltpu.SemaphoreType.DMA((4,)),
                pltpu.SemaphoreType.DMA((4,)),
                *pairs,
            ],
            compiler_params=pltpu.CompilerParams(
                collective_id=0, has_side_effects=True, vmem_limit_bytes=44 * 2**20
            ),
            name="exchange",
        )(*(in_hbm(operand) for operand in operands))
        w = pl.pallas_call(
            last_kernel,
            out_shape=jax.ShapeDtypeStruct((BLOCKS * BLOCK, N), F32),
            in_specs=[vmem, vmem],
            out_specs=any_space,
            scratch_shapes=[pltpu.VMEM((BLOCKS * BLOCK, N), F32), pltpu.SemaphoreType.DMA((BLOCKS,))],
            compiler_params=pltpu.CompilerParams(vmem_limit_bytes=24 * 2**20),
            name="last",
        )(h5.reshape(BLOCKS * BLOCK, N), last_a)
        return jnp.transpose(w.reshape(batch, S, S, N), (0, 3, 1, 2))

    spec_field = P("fields", None, "row", "col")
    spec_factor = P("fields", None)
    return jax.shard_map(
        local_apply,
        mesh=mesh,
        in_specs=(spec_field, spec_factor, spec_factor, spec_factor, P(("fields", "row"), "col", None)),
        out_specs=spec_field,
        check_vma=False,
    )
```

```python
import functools

import jax
import jax.numpy as jnp
from jax import lax
from jax.experimental import pallas as pl
from jax.experimental.pallas import tpu as pltpu
from jax.sharding import PartitionSpec as P

MESH = pl.DeviceIdType.MESH
N = 128
S = 32
H = 16
FINE = 8
PER = S // FINE
ROUNDS = 8
EARLY = 2
LATE = 1
LEAD = 4
GROUP = 4
BLOCKS, BLOCK = 8, 4096
F32, BF16 = jnp.float32, jnp.bfloat16
PEERS = (1, 2, 3)


def xor(value, bits):
    if bits == 0:
        return value
    if bits == 1:
        return value + 1 - 2 * lax.rem(value, 2)
    if bits == 2:
        return lax.rem(value + 2, 4)
    return 3 - value


def chunk(index, size=S):
    return pl.ds(pl.multiple_of(index * size, size), size)


def dot(lhs, rhs, lhs_dim, rhs_dim):
    return lax.dot_general(lhs, rhs, (((lhs_dim,), (rhs_dim,)), ((), ())), preferred_element_type=F32)


def exchange_kernel(
    u_ref, a_hbm, b_hbm, c_hbm, d_ref, o_ref, a_out,
    fine_in, tens, cols, rets, fine_out, front, rear, diag, diag_t,
    a_ref, b_ref, c_ref, b_t, c_t, factor_sem, d_send, d_recv, *sems,
):
    row, col = lax.axis_index("row"), lax.axis_index("col")

    def row_peer(dr):
        return {"row": xor(row, dr), "col": col} if dr else None

    def col_peer(dc):
        return {"row": row, "col": xor(col, dc)} if dc else None

    def copy(src, dst, send, recv, peer):
        if not peer:
            return pltpu.make_async_copy(src, dst, recv)
        return pltpu.make_async_remote_copy(
            src_ref=src, dst_ref=dst, send_sem=send, recv_sem=recv, device_id=peer, device_id_type=MESH
        )

    def paired(which, index, offset):
        return sems[2 * which].at[index, offset], sems[2 * which + 1].at[index, offset]

    def row_round(t, dr):
        src = u_ref.at[(t + EARLY) * 4 + xor(row, dr)]
        return copy(src, tens.at[t, chunk(row)], *paired(0, t, dr), row_peer(dr))

    def row_fine(unit, dr):
        t, z = lax.div(unit, PER), lax.rem(unit, PER)
        src = u_ref.at[t * 4 + xor(row, dr), :, chunk(z, FINE), :]
        return copy(src, fine_in.at[unit, chunk(row)], *paired(1, unit, dr), row_peer(dr))

    def go_round(t, dc):
        dst = cols.at[t + EARLY, :, chunk(col), :]
        return copy(tens.at[t, chunk(xor(col, dc))], dst, *paired(2, t, dc), col_peer(dc))

    def go_fine(unit, dc):
        t, z = lax.div(unit, PER), lax.rem(unit, PER)
        dst = cols.at[t, :, chunk(col * PER + z, FINE), :]
        return copy(fine_in.at[unit, chunk(xor(col, dc))], dst, *paired(3, unit, dc), col_peer(dc))

    def back_round(t, dc):
        src = cols.at[t, :, chunk(xor(col, dc)), :]
        return copy(src, rets.at[t, chunk(col)], *paired(4, t, dc), col_peer(dc))

    def back_fine(unit, dc):
        t, z = lax.div(unit, PER) + ROUNDS - LATE, lax.rem(unit, PER)
        src = cols.at[t, :, chunk(xor(col, dc) * PER + z, FINE), :]
        return copy(src, fine_out.at[unit, chunk(col)], *paired(5, unit, dc), col_peer(dc))

    def home_round(t, dr):
        dst = o_ref.at[t * 4 + row]
        return copy(rets.at[t, chunk(xor(row, dr))], dst, *paired(6, t, dr), row_peer(dr))

    def home_fine(unit, dr):
        t, z = lax.div(unit, PER) + ROUNDS - LATE, lax.rem(unit, PER)
        dst = o_ref.at[t * 4 + row, :, chunk(z, FINE), :]
        return copy(fine_out.at[unit, chunk(xor(row, dr))], dst, *paired(7, unit, dr), row_peer(dr))

    def start(kind, index):
        for peer in (0, 3, 2, 1) if kind in (row_round, row_fine, home_round, home_fine) else (1, 2, 3, 0):
            kind(index, peer).start()

    def arrive(kind, index):
        kind(index, 0).wait()
        for peer in PEERS:
            kind(index, peer).wait_recv()

    barrier = pltpu.get_barrier_semaphore()
    for peer in PEERS:
        pl.semaphore_signal(barrier, inc=1, device_id=row_peer(peer), device_id_type=MESH)
        pl.semaphore_signal(barrier, inc=1, device_id=col_peer(peer), device_id_type=MESH)
    pl.semaphore_wait(barrier, 2 * len(PEERS))

    @pl.loop(0, PER * EARLY)
    def _(unit):
        start(row_fine, unit)

    own_d, far_d = diag.at[chunk(row, S * S)], diag.at[chunk(xor(row, 2), S * S)]
    keep_d = copy(d_ref, own_d, None, d_recv.at[0], None)
    cross_d = copy(d_ref, own_d, d_send.at[1], d_recv.at[1], row_peer(2))
    near_d = copy(d_ref, own_d, d_send.at[2], d_recv.at[2], row_peer(1))
    pass_d = copy(far_d, far_d, d_send.at[3], d_recv.at[3], row_peer(1))
    for start_d in (cross_d, near_d, keep_d):
        start_d.start()

    @pl.loop(0, ROUNDS - EARLY)
    def _(t):
        start(row_round, t)

    factors = [
        pltpu.make_async_copy(a_hbm, a_ref, factor_sem.at[0]),
        pltpu.make_async_copy(b_hbm, b_ref, factor_sem.at[1]),
        pltpu.make_async_copy(c_hbm, c_ref, factor_sem.at[2]),
        pltpu.make_async_copy(a_hbm, a_out, factor_sem.at[3]),
    ]
    for factor in factors:
        factor.start()
    for factor in factors:
        factor.wait()
    b_t[...] = b_ref[...].T
    c_t[...] = c_ref[...].T

    def swapped(matrix, height):
        @pl.loop(0, height // GROUP)
        def _(step):
            lines = [pl.ds(step * GROUP + n, N, stride=height) for n in range(GROUP)]
            side = jnp.concatenate([front[line, :].astype(BF16) for line in lines], axis=1)
            both = dot(matrix[...], side, 1, 0)
            for n, line in enumerate(lines):
                rear[line, :] = both[:, n * N:(n + 1) * N]

    def first_two(view, height):
        @pl.loop(0, 4)
        def _(q):
            block = view[chunk(q)].reshape(S * height, N)
            front[chunk(q, S * height), :] = dot(block, a_ref[...], 1, 1)

        swapped(b_ref, height)

    def fifth(view, height):
        @pl.loop(0, 4)
        def _(q):
            front[chunk(q, S * height), :] = view[chunk(q)].reshape(S * height, N).astype(F32)

        swapped(b_t, height)

    def rounded(view, height):
        @pl.loop(0, 4)
        def _(q):
            view[chunk(q)] = rear[chunk(q, S * height), :].reshape(S, height, N).astype(BF16)

    def fine(here, there, buffer, work, unit):
        arrive(here, unit)
        work(buffer.at[unit], FINE)
        rounded(buffer.at[unit], FINE)
        start(there, unit)

    def whole(here, there, buffer, work, t):
        arrive(here, t)

        @pl.loop(0, S // H)
        def _(half):
            view = buffer.at[t, :, chunk(half, H), :]
            work(view, H)
            rounded(view, H)

        start(there, t)

    def middle(t, early, late):
        if early:
            for n in range(PER):
                arrive(go_fine, PER * t + n)
        else:
            arrive(go_round, t - EARLY)

        @pl.loop(0, S // GROUP)
        def _(step):
            def side(buffer):
                return jnp.concatenate([buffer[step * GROUP + n] for n in range(GROUP)], axis=1)

            h3 = (dot(c_ref[...], side(cols.at[t]), 1, 0) * side(diag_t)).astype(BF16)
            h4 = dot(c_t[...], h3, 1, 0).astype(BF16)
            for n in range(GROUP):
                cols[t, step * GROUP + n] = h4[:, n * N:(n + 1) * N]

        if late:
            for n in range(PER):
                start(back_fine, PER * (t - ROUNDS + LATE) + n)
        else:
            start(back_round, t)

    pl.loop(0, PER * EARLY)(functools.partial(fine, row_fine, go_fine, fine_in, first_two))
    cross_d.wait_recv()
    pass_d.start()
    keep_d.wait()
    near_d.wait_recv()
    pass_d.wait_recv()

    @pl.loop(0, S)
    def _(j):
        diag_t[j] = diag[pl.ds(j, N, stride=S), :].T

    first_round = functools.partial(whole, row_round, go_round, tens, first_two)
    fifth_round = functools.partial(whole, back_round, home_round, rets, fifth)

    def body(t, early=False, late=False, firsts=False, fifths=True):
        middle(t, early, late)
        if firsts:
            first_round(t + LEAD - EARLY)
        if fifths:
            fifth_round(t - 2)

    pl.loop(0, LEAD - EARLY)(first_round)
    pl.loop(0, 2)(functools.partial(body, early=True, firsts=True, fifths=False))
    pl.loop(2, 4)(functools.partial(body, firsts=True))
    pl.loop(4, 7)(body)
    pl.loop(7, 8)(functools.partial(body, late=True))
    pl.loop(6, 7)(fifth_round)
    pl.loop(0, PER * LATE)(functools.partial(fine, back_fine, home_fine, fine_out, fifth))

    def finish(kinds, index):
        for kind in kinds:
            if kind in (home_round, home_fine):
                arrive(kind, index)
            for peer in PEERS:
                kind(index, peer).wait_send()

    for sent in (cross_d, near_d, pass_d):
        sent.wait_send()
    pl.loop(0, PER * EARLY)(functools.partial(finish, (row_fine, go_fine)))
    pl.loop(0, ROUNDS - EARLY)(functools.partial(finish, (row_round, go_round)))
    pl.loop(0, ROUNDS - LATE)(functools.partial(finish, (back_round, home_round)))
    pl.loop(0, PER * LATE)(functools.partial(finish, (back_fine, home_fine)))


def last_kernel(h_ref, a_ref, w_ref, out, sem):
    def store(n):
        rows = chunk(n, BLOCK)
        return pltpu.make_async_copy(out.at[rows], w_ref.at[rows], sem.at[n])

    @pl.loop(0, BLOCKS)
    def _(n):
        rows = chunk(n, BLOCK)
        out[rows, :] = dot(h_ref[rows, :], a_ref[...], 1, 0)
        store(n).start()

    @pl.loop(0, BLOCKS)
    def _(n):
        store(n).wait()


def solution(mesh):
    def local_apply(field_u, fac_a, fac_b, fac_c, diag_d):
        batch = field_u.shape[0]
        any_space = pl.BlockSpec(memory_space=pl.ANY)
        vmem = pl.BlockSpec(memory_space=pltpu.VMEM)

        def in_hbm(array):
            return pltpu.with_memory_space_constraint(array, pltpu.HBM)

        operands = (jnp.transpose(field_u, (0, 2, 3, 1)), fac_a, fac_b, fac_c, diag_d.reshape(S * S, N))
        counts = (ROUNDS - EARLY, PER * EARLY) * 2 + (ROUNDS - LATE, PER * LATE) * 2
        pairs = [pltpu.SemaphoreType.DMA((n, 4)) for n in counts for _ in range(2)]
        h5, last_a = pl.pallas_call(
            exchange_kernel,
            out_shape=(pltpu.VMEM((batch, S, S, N), BF16), pltpu.VMEM((N, N), BF16)),
            in_specs=[any_space] * 5,
            out_specs=(any_space, any_space),
            scratch_shapes=[
                pltpu.VMEM((PER * EARLY, N, FINE, N), BF16),
                pltpu.VMEM((ROUNDS - EARLY, N, S, N), BF16),
                pltpu.VMEM((ROUNDS, S, N, N), BF16),
                pltpu.VMEM((ROUNDS - LATE, N, S, N), BF16),
                pltpu.VMEM((PER * LATE, N, FINE, N), BF16),
                pltpu.VMEM((N * H, N), F32),
                pltpu.VMEM((N * H, N), F32),
                pltpu.VMEM((N * S, N), F32),
                pltpu.VMEM((S, N, N), F32),
                pltpu.VMEM((N, N), BF16),
                pltpu.VMEM((N, N), BF16),
                pltpu.VMEM((N, N), BF16),
                pltpu.VMEM((N, N), BF16),
                pltpu.VMEM((N, N), BF16),
                pltpu.SemaphoreType.DMA((4,)),
                pltpu.SemaphoreType.DMA((4,)),
                pltpu.SemaphoreType.DMA((4,)),
                *pairs,
            ],
            compiler_params=pltpu.CompilerParams(
                collective_id=0, has_side_effects=True, vmem_limit_bytes=44 * 2**20
            ),
            name="exchange",
        )(*(in_hbm(operand) for operand in operands))
        w = pl.pallas_call(
            last_kernel,
            out_shape=jax.ShapeDtypeStruct((BLOCKS * BLOCK, N), F32),
            in_specs=[vmem, vmem],
            out_specs=any_space,
            scratch_shapes=[pltpu.VMEM((BLOCKS * BLOCK, N), F32), pltpu.SemaphoreType.DMA((BLOCKS,))],
            compiler_params=pltpu.CompilerParams(vmem_limit_bytes=24 * 2**20),
            name="last",
        )(h5.reshape(BLOCKS * BLOCK, N), last_a)
        return jnp.transpose(w.reshape(batch, S, S, N), (0, 3, 1, 2))

    spec_field = P("fields", None, "row", "col")
    spec_factor = P("fields", None)
    return jax.shard_map(
        local_apply,
        mesh=mesh,
        in_specs=(spec_field, spec_factor, spec_factor, spec_factor, P(("fields", "row"), "col", None)),
        out_specs=spec_field,
        check_vma=False,
    )
```

```python
import functools

import jax
import jax.numpy as jnp
from jax import lax
from jax.experimental import pallas as pl
from jax.experimental.pallas import tpu as pltpu
from jax.sharding import PartitionSpec as P

MESH = pl.DeviceIdType.MESH
N = 128
S = 32
H = 16
FINE = 8
PER = S // FINE
ROUNDS = 8
EARLY = 1
LATE = 1
LEAD = 4
GROUP = 4
BLOCKS, BLOCK = 16, 2048
F32, BF16 = jnp.float32, jnp.bfloat16
PEERS = (1, 2, 3)


def xor(value, bits):
    if bits == 0:
        return value
    if bits == 1:
        return value + 1 - 2 * lax.rem(value, 2)
    if bits == 2:
        return lax.rem(value + 2, 4)
    return 3 - value


def chunk(index, size=S):
    return pl.ds(pl.multiple_of(index * size, size), size)


def dot(lhs, rhs, lhs_dim, rhs_dim):
    return lax.dot_general(lhs, rhs, (((lhs_dim,), (rhs_dim,)), ((), ())), preferred_element_type=F32)


def exchange_kernel(
    u_ref, a_hbm, b_hbm, c_hbm, d_ref, o_ref, a_out,
    fine_in, tens, cols, rets, fine_out, front, rear, diag, diag_t,
    a_ref, b_ref, c_ref, b_t, c_t, factor_sem, d_send, d_recv, *sems,
):
    row, col = lax.axis_index("row"), lax.axis_index("col")

    def row_peer(dr):
        return {"row": xor(row, dr), "col": col} if dr else None

    def col_peer(dc):
        return {"row": row, "col": xor(col, dc)} if dc else None

    def copy(src, dst, send, recv, peer):
        if not peer:
            return pltpu.make_async_copy(src, dst, recv)
        return pltpu.make_async_remote_copy(
            src_ref=src, dst_ref=dst, send_sem=send, recv_sem=recv, device_id=peer, device_id_type=MESH
        )

    def paired(which, index, offset):
        return sems[2 * which].at[index, offset], sems[2 * which + 1].at[index, offset]

    def row_round(t, dr):
        src = u_ref.at[(t + EARLY) * 4 + xor(row, dr)]
        return copy(src, tens.at[t, chunk(row)], *paired(0, t, dr), row_peer(dr))

    def row_fine(unit, dr):
        t, z = lax.div(unit, PER), lax.rem(unit, PER)
        src = u_ref.at[t * 4 + xor(row, dr), :, chunk(z, FINE), :]
        return copy(src, fine_in.at[unit, chunk(row)], *paired(1, unit, dr), row_peer(dr))

    def go_round(t, dc):
        dst = cols.at[t + EARLY, col]
        return copy(tens.at[t, chunk(xor(col, dc))], dst, *paired(2, t, dc), col_peer(dc))

    def go_fine(unit, dc):
        t, z = lax.div(unit, PER), lax.rem(unit, PER)
        dst = cols.at[t, col, :, chunk(z, FINE), :]
        return copy(fine_in.at[unit, chunk(xor(col, dc))], dst, *paired(3, unit, dc), col_peer(dc))

    def back_round(t, dc):
        src = cols.at[t, xor(col, dc)]
        return copy(src, rets.at[t, chunk(col)], *paired(4, t, dc), col_peer(dc))

    def back_fine(unit, dc):
        t, z = lax.div(unit, PER) + ROUNDS - LATE, lax.rem(unit, PER)
        src = cols.at[t, xor(col, dc), :, chunk(z, FINE), :]
        return copy(src, fine_out.at[unit, chunk(col)], *paired(5, unit, dc), col_peer(dc))

    def home_round(t, dr):
        dst = o_ref.at[t * 4 + row]
        return copy(rets.at[t, chunk(xor(row, dr))], dst, *paired(6, t, dr), row_peer(dr))

    def home_fine(unit, dr):
        t, z = lax.div(unit, PER) + ROUNDS - LATE, lax.rem(unit, PER)
        dst = o_ref.at[t * 4 + row, :, chunk(z, FINE), :]
        return copy(fine_out.at[unit, chunk(xor(row, dr))], dst, *paired(7, unit, dr), row_peer(dr))

    def start(kind, index):
        for peer in (0, 3, 2, 1) if kind in (row_round, row_fine, home_round, home_fine) else (1, 2, 3, 0):
            kind(index, peer).start()

    def arrive(kind, index):
        kind(index, 0).wait()
        for peer in PEERS:
            kind(index, peer).wait_recv()

    barrier = pltpu.get_barrier_semaphore()
    for peer in PEERS:
        pl.semaphore_signal(barrier, inc=1, device_id=row_peer(peer), device_id_type=MESH)
        pl.semaphore_signal(barrier, inc=1, device_id=col_peer(peer), device_id_type=MESH)
    pl.semaphore_wait(barrier, 2 * len(PEERS))

    @pl.loop(0, PER * EARLY)
    def _(unit):
        start(row_fine, unit)

    start(row_round, 0)

    own_d, far_d = diag.at[chunk(row, S * S)], diag.at[chunk(xor(row, 2), S * S)]
    keep_d = copy(d_ref, own_d, None, d_recv.at[0], None)
    cross_d = copy(d_ref, own_d, d_send.at[1], d_recv.at[1], row_peer(2))
    near_d = copy(d_ref, own_d, d_send.at[2], d_recv.at[2], row_peer(1))
    pass_d = copy(far_d, far_d, d_send.at[3], d_recv.at[3], row_peer(1))
    for start_d in (cross_d, near_d, keep_d):
        start_d.start()

    @pl.loop(1, ROUNDS - EARLY)
    def _(t):
        start(row_round, t)

    factors = [
        pltpu.make_async_copy(a_hbm, a_ref, factor_sem.at[0]),
        pltpu.make_async_copy(b_hbm, b_ref, factor_sem.at[1]),
        pltpu.make_async_copy(c_hbm, c_ref, factor_sem.at[2]),
        pltpu.make_async_copy(a_hbm, a_out, factor_sem.at[3]),
    ]
    for factor in factors:
        factor.start()
    for factor in factors:
        factor.wait()
    b_t[...] = b_ref[...].T
    c_t[...] = c_ref[...].T

    def swapped(matrix, height):
        @pl.loop(0, height // GROUP)
        def _(step):
            lines = [pl.ds(step * GROUP + n, N, stride=height) for n in range(GROUP)]
            side = jnp.concatenate([front[line, :].astype(BF16) for line in lines], axis=1)
            both = dot(matrix[...], side, 1, 0)
            for n, line in enumerate(lines):
                rear[line, :] = both[:, n * N:(n + 1) * N]

    def first_two(view, height):
        @pl.loop(0, 4)
        def _(q):
            block = view[chunk(q)].reshape(S * height, N)
            front[chunk(q, S * height), :] = dot(block, a_ref[...], 1, 1)

        swapped(b_ref, height)

    def fifth(view, height):
        @pl.loop(0, 4)
        def _(q):
            front[chunk(q, S * height), :] = view[chunk(q)].reshape(S * height, N).astype(F32)

        swapped(b_t, height)

    def rounded(view, height):
        @pl.loop(0, 4)
        def _(q):
            view[chunk(q)] = rear[chunk(q, S * height), :].reshape(S, height, N).astype(BF16)

    def fine(here, there, buffer, work, unit):
        arrive(here, unit)
        work(buffer.at[unit], FINE)
        rounded(buffer.at[unit], FINE)
        start(there, unit)

    def whole(here, there, buffer, work, t):
        arrive(here, t)

        @pl.loop(0, S // H)
        def _(half):
            view = buffer.at[t, :, chunk(half, H), :]
            work(view, H)
            rounded(view, H)

        start(there, t)

    def middle(t, early, late):
        if early:
            for n in range(PER):
                arrive(go_fine, PER * t + n)
        else:
            arrive(go_round, t - EARLY)

        @pl.loop(0, S // GROUP)
        def _(step):
            def slab(j):
                return jnp.concatenate([cols[t, c, j] for c in range(4)], axis=0)

            js = [step * GROUP + n for n in range(GROUP)]
            h2 = jnp.concatenate([slab(j) for j in js], axis=1)
            scale = jnp.concatenate([diag_t[j] for j in js], axis=1)
            h3 = (dot(c_ref[...], h2, 1, 0) * scale).astype(BF16)
            h4 = dot(c_t[...], h3, 1, 0).astype(BF16)
            for n, j in enumerate(js):
                for c in range(4):
                    cols[t, c, j] = h4[c * S:(c + 1) * S, n * N:(n + 1) * N]

        if late:
            for n in range(PER):
                start(back_fine, PER * (t - ROUNDS + LATE) + n)
        else:
            start(back_round, t)

    first_round = functools.partial(whole, row_round, go_round, tens, first_two)
    fifth_round = functools.partial(whole, back_round, home_round, rets, fifth)

    pl.loop(0, PER * EARLY)(functools.partial(fine, row_fine, go_fine, fine_in, first_two))
    pl.loop(0, 1)(first_round)
    cross_d.wait_recv()
    pass_d.start()
    keep_d.wait()
    near_d.wait_recv()
    pass_d.wait_recv()

    @pl.loop(0, S)
    def _(j):
        diag_t[j] = diag[pl.ds(j, N, stride=S), :].T

    def body(t, early=False, late=False, firsts=False, fifths=True):
        middle(t, early, late)
        if firsts:
            first_round(t + LEAD - EARLY)
        if fifths:
            fifth_round(t - 2)

    pl.loop(1, LEAD - EARLY)(first_round)
    pl.loop(0, 1)(functools.partial(body, early=True, firsts=True, fifths=False))
    pl.loop(1, 2)(functools.partial(body, firsts=True, fifths=False))
    pl.loop(2, 4)(functools.partial(body, firsts=True))
    pl.loop(4, 7)(body)
    pl.loop(7, 8)(functools.partial(body, late=True))
    pl.loop(6, 7)(fifth_round)
    pl.loop(0, PER * LATE)(functools.partial(fine, back_fine, home_fine, fine_out, fifth))

    def finish(kinds, index):
        for kind in kinds:
            if kind in (home_round, home_fine):
                arrive(kind, index)
            for peer in PEERS:
                kind(index, peer).wait_send()

    for sent in (cross_d, near_d, pass_d):
        sent.wait_send()
    pl.loop(0, PER * EARLY)(functools.partial(finish, (row_fine, go_fine)))
    pl.loop(0, ROUNDS - EARLY)(functools.partial(finish, (row_round, go_round)))
    pl.loop(0, ROUNDS - LATE)(functools.partial(finish, (back_round, home_round)))
    pl.loop(0, PER * LATE)(functools.partial(finish, (back_fine, home_fine)))


def last_kernel(h_ref, a_ref, w_ref, out, sem):
    def store(n):
        rows = chunk(n, BLOCK)
        return pltpu.make_async_copy(out.at[rows], w_ref.at[rows], sem.at[n])

    @pl.loop(0, BLOCKS)
    def _(n):
        rows = chunk(n, BLOCK)
        out[rows, :] = dot(h_ref[rows, :], a_ref[...], 1, 0)
        store(n).start()

    @pl.loop(0, BLOCKS)
    def _(n):
        store(n).wait()


def solution(mesh):
    def local_apply(field_u, fac_a, fac_b, fac_c, diag_d):
        batch = field_u.shape[0]
        any_space = pl.BlockSpec(memory_space=pl.ANY)
        vmem = pl.BlockSpec(memory_space=pltpu.VMEM)

        def in_hbm(array):
            return pltpu.with_memory_space_constraint(array, pltpu.HBM)

        operands = (jnp.transpose(field_u, (0, 2, 3, 1)), fac_a, fac_b, fac_c, diag_d.reshape(S * S, N))
        counts = (ROUNDS - EARLY, PER * EARLY) * 2 + (ROUNDS - LATE, PER * LATE) * 2
        pairs = [pltpu.SemaphoreType.DMA((n, 4)) for n in counts for _ in range(2)]
        h5, last_a = pl.pallas_call(
            exchange_kernel,
            out_shape=(pltpu.VMEM((batch, S, S, N), BF16), pltpu.VMEM((N, N), BF16)),
            in_specs=[any_space] * 5,
            out_specs=(any_space, any_space),
            scratch_shapes=[
                pltpu.VMEM((PER * EARLY, N, FINE, N), BF16),
                pltpu.VMEM((ROUNDS - EARLY, N, S, N), BF16),
                pltpu.VMEM((ROUNDS, 4, S, S, N), BF16),
                pltpu.VMEM((ROUNDS - LATE, N, S, N), BF16),
                pltpu.VMEM((PER * LATE, N, FINE, N), BF16),
                pltpu.VMEM((N * H, N), F32),
                pltpu.VMEM((N * H, N), F32),
                pltpu.VMEM((N * S, N), F32),
                pltpu.VMEM((S, N, N), F32),
                pltpu.VMEM((N, N), BF16),
                pltpu.VMEM((N, N), BF16),
                pltpu.VMEM((N, N), BF16),
                pltpu.VMEM((N, N), BF16),
                pltpu.VMEM((N, N), BF16),
                pltpu.SemaphoreType.DMA((4,)),
                pltpu.SemaphoreType.DMA((4,)),
                pltpu.SemaphoreType.DMA((4,)),
                *pairs,
            ],
            compiler_params=pltpu.CompilerParams(
                collective_id=0, has_side_effects=True, vmem_limit_bytes=44 * 2**20
            ),
            name="exchange",
        )(*(in_hbm(operand) for operand in operands))
        w = pl.pallas_call(
            last_kernel,
            out_shape=jax.ShapeDtypeStruct((BLOCKS * BLOCK, N), F32),
            in_specs=[vmem, vmem],
            out_specs=any_space,
            scratch_shapes=[pltpu.VMEM((BLOCKS * BLOCK, N), F32), pltpu.SemaphoreType.DMA((BLOCKS,))],
            compiler_params=pltpu.CompilerParams(vmem_limit_bytes=24 * 2**20),
            name="last",
        )(h5.reshape(BLOCKS * BLOCK, N), last_a)
        return jnp.transpose(w.reshape(batch, S, S, N), (0, 3, 1, 2))

    spec_field = P("fields", None, "row", "col")
    spec_factor = P("fields", None)
    return jax.shard_map(
        local_apply,
        mesh=mesh,
        in_specs=(spec_field, spec_factor, spec_factor, spec_factor, P(("fields", "row"), "col", None)),
        out_specs=spec_field,
        check_vma=False,
    )
```

```python
import functools

import jax
import jax.numpy as jnp
from jax import lax
from jax.experimental import pallas as pl
from jax.experimental.pallas import tpu as pltpu
from jax.sharding import PartitionSpec as P

MESH = pl.DeviceIdType.MESH
N = 128
S = 32
H = 16
FINE = 8
PER = S // FINE
ROUNDS = 8
EARLY = 1
LATE = 1
GROUP = 4
BLOCKS, BLOCK = 16, 2048
F32, BF16 = jnp.float32, jnp.bfloat16
PEERS = (1, 2, 3)


def xor(value, bits):
    if bits == 0:
        return value
    if bits == 1:
        return value + 1 - 2 * lax.rem(value, 2)
    if bits == 2:
        return lax.rem(value + 2, 4)
    return 3 - value


def chunk(index, size=S):
    return pl.ds(pl.multiple_of(index * size, size), size)


def dot(lhs, rhs, lhs_dim, rhs_dim):
    return lax.dot_general(lhs, rhs, (((lhs_dim,), (rhs_dim,)), ((), ())), preferred_element_type=F32)


def exchange_kernel(
    u_ref, a_hbm, b_hbm, c_hbm, d_ref, o_ref, a_out,
    fine_in, tens, cols, rets, fine_out, front, rear, diag, diag_t,
    a_ref, b_ref, c_ref, b_t, c_t, factor_sem, d_send, d_recv, *sems,
):
    row, col = lax.axis_index("row"), lax.axis_index("col")

    def row_peer(dr):
        return {"row": xor(row, dr), "col": col} if dr else None

    def col_peer(dc):
        return {"row": row, "col": xor(col, dc)} if dc else None

    def copy(src, dst, send, recv, peer):
        if not peer:
            return pltpu.make_async_copy(src, dst, recv)
        return pltpu.make_async_remote_copy(
            src_ref=src, dst_ref=dst, send_sem=send, recv_sem=recv, device_id=peer, device_id_type=MESH
        )

    def paired(which, index, offset):
        return sems[2 * which].at[index, offset], sems[2 * which + 1].at[index, offset]

    def row_round(t, dr):
        src = u_ref.at[(t + EARLY) * 4 + xor(row, dr)]
        return copy(src, tens.at[t, chunk(row)], *paired(0, t, dr), row_peer(dr))

    def row_fine(unit, dr):
        t, z = lax.div(unit, PER), lax.rem(unit, PER)
        src = u_ref.at[t * 4 + xor(row, dr), :, chunk(z, FINE), :]
        return copy(src, fine_in.at[unit, chunk(row)], *paired(1, unit, dr), row_peer(dr))

    def go_round(t, dc):
        dst = cols.at[t + EARLY, col]
        return copy(tens.at[t, chunk(xor(col, dc))], dst, *paired(2, t, dc), col_peer(dc))

    def go_fine(unit, dc):
        t, z = lax.div(unit, PER), lax.rem(unit, PER)
        dst = cols.at[t, col, :, chunk(z, FINE), :]
        return copy(fine_in.at[unit, chunk(xor(col, dc))], dst, *paired(3, unit, dc), col_peer(dc))

    def back_round(t, dc):
        src = cols.at[t, xor(col, dc)]
        return copy(src, rets.at[t, chunk(col)], *paired(4, t, dc), col_peer(dc))

    def back_fine(unit, dc):
        t, z = lax.div(unit, PER) + ROUNDS - LATE, lax.rem(unit, PER)
        src = cols.at[t, xor(col, dc), :, chunk(z, FINE), :]
        return copy(src, fine_out.at[unit, chunk(col)], *paired(5, unit, dc), col_peer(dc))

    def home_round(t, dr):
        dst = o_ref.at[t * 4 + row]
        return copy(rets.at[t, chunk(xor(row, dr))], dst, *paired(6, t, dr), row_peer(dr))

    def home_fine(unit, dr):
        t, z = lax.div(unit, PER) + ROUNDS - LATE, lax.rem(unit, PER)
        dst = o_ref.at[t * 4 + row, :, chunk(z, FINE), :]
        return copy(fine_out.at[unit, chunk(xor(row, dr))], dst, *paired(7, unit, dr), row_peer(dr))

    def start(kind, index):
        for peer in (0, 3, 2, 1) if kind in (row_round, row_fine, home_round, home_fine) else (1, 2, 3, 0):
            kind(index, peer).start()

    def arrive(kind, index):
        kind(index, 0).wait()
        for peer in PEERS:
            kind(index, peer).wait_recv()

    barrier = pltpu.get_barrier_semaphore()
    for peer in PEERS:
        pl.semaphore_signal(barrier, inc=1, device_id=row_peer(peer), device_id_type=MESH)
        pl.semaphore_signal(barrier, inc=1, device_id=col_peer(peer), device_id_type=MESH)
    pl.semaphore_wait(barrier, 2 * len(PEERS))

    @pl.loop(0, PER * EARLY)
    def _(unit):
        start(row_fine, unit)

    start(row_round, 0)

    own_d, far_d = diag.at[chunk(row, S * S)], diag.at[chunk(xor(row, 2), S * S)]
    keep_d = copy(d_ref, own_d, None, d_recv.at[0], None)
    cross_d = copy(d_ref, own_d, d_send.at[1], d_recv.at[1], row_peer(2))
    near_d = copy(d_ref, own_d, d_send.at[2], d_recv.at[2], row_peer(1))
    pass_d = copy(far_d, far_d, d_send.at[3], d_recv.at[3], row_peer(1))
    for start_d in (cross_d, near_d, keep_d):
        start_d.start()

    @pl.loop(1, ROUNDS - EARLY)
    def _(t):
        start(row_round, t)

    factors = [
        pltpu.make_async_copy(a_hbm, a_ref, factor_sem.at[0]),
        pltpu.make_async_copy(b_hbm, b_ref, factor_sem.at[1]),
        pltpu.make_async_copy(c_hbm, c_ref, factor_sem.at[2]),
        pltpu.make_async_copy(a_hbm, a_out, factor_sem.at[3]),
    ]
    for factor in factors:
        factor.start()
    for factor in factors:
        factor.wait()
    b_t[...] = b_ref[...].T
    c_t[...] = c_ref[...].T

    def swapped(matrix, height):
        @pl.loop(0, height // GROUP)
        def _(step):
            lines = [pl.ds(step * GROUP + n, N, stride=height) for n in range(GROUP)]
            side = jnp.concatenate([front[line, :].astype(BF16) for line in lines], axis=1)
            both = dot(matrix[...], side, 1, 0)
            for n, line in enumerate(lines):
                rear[line, :] = both[:, n * N:(n + 1) * N]

    def first_two(view, height):
        @pl.loop(0, 4)
        def _(q):
            block = view[chunk(q)].reshape(S * height, N)
            front[chunk(q, S * height), :] = dot(block, a_ref[...], 1, 1)

        swapped(b_ref, height)

    def fifth(view, height):
        @pl.loop(0, 4)
        def _(q):
            front[chunk(q, S * height), :] = view[chunk(q)].reshape(S * height, N).astype(F32)

        swapped(b_t, height)

    def rounded(view, height):
        @pl.loop(0, 4)
        def _(q):
            view[chunk(q)] = rear[chunk(q, S * height), :].reshape(S, height, N).astype(BF16)

    def fine(here, there, buffer, work, unit):
        arrive(here, unit)
        work(buffer.at[unit], FINE)
        rounded(buffer.at[unit], FINE)
        start(there, unit)

    def whole(here, there, buffer, work, t):
        arrive(here, t)

        @pl.loop(0, S // H)
        def _(half):
            view = buffer.at[t, :, chunk(half, H), :]
            work(view, H)
            rounded(view, H)

        start(there, t)

    def middle(t, early, late):
        if early:
            for n in range(PER):
                arrive(go_fine, PER * t + n)
        else:
            arrive(go_round, t - EARLY)

        @pl.loop(0, S // GROUP)
        def _(step):
            def slab(j):
                return jnp.concatenate([cols[t, c, j] for c in range(4)], axis=0)

            js = [step * GROUP + n for n in range(GROUP)]
            h2 = jnp.concatenate([slab(j) for j in js], axis=1)
            scale = jnp.concatenate([diag_t[j] for j in js], axis=1)
            h3 = (dot(c_ref[...], h2, 1, 0) * scale).astype(BF16)
            h4 = dot(c_t[...], h3, 1, 0).astype(BF16)
            for n, j in enumerate(js):
                for c in range(4):
                    cols[t, c, j] = h4[c * S:(c + 1) * S, n * N:(n + 1) * N]

        if late:
            for n in range(PER):
                start(back_fine, PER * (t - ROUNDS + LATE) + n)
        else:
            start(back_round, t)

    first_round = functools.partial(whole, row_round, go_round, tens, first_two)
    fifth_round = functools.partial(whole, back_round, home_round, rets, fifth)

    pl.loop(0, PER * EARLY)(functools.partial(fine, row_fine, go_fine, fine_in, first_two))
    pl.loop(0, 1)(first_round)
    cross_d.wait_recv()
    pass_d.start()
    keep_d.wait()
    near_d.wait_recv()
    pass_d.wait_recv()

    @pl.loop(0, S)
    def _(j):
        diag_t[j] = diag[pl.ds(j, N, stride=S), :].T

    pl.loop(1, ROUNDS - EARLY)(first_round)
    pl.loop(0, EARLY)(functools.partial(middle, early=True, late=False))
    pl.loop(EARLY, ROUNDS - LATE)(functools.partial(middle, early=False, late=False))
    pl.loop(ROUNDS - LATE, ROUNDS)(functools.partial(middle, early=False, late=True))
    pl.loop(0, ROUNDS - LATE)(fifth_round)
    pl.loop(0, PER * LATE)(functools.partial(fine, back_fine, home_fine, fine_out, fifth))

    def finish(kinds, index):
        for kind in kinds:
            if kind in (home_round, home_fine):
                arrive(kind, index)
            for peer in PEERS:
                kind(index, peer).wait_send()

    for sent in (cross_d, near_d, pass_d):
        sent.wait_send()
    pl.loop(0, PER * EARLY)(functools.partial(finish, (row_fine, go_fine)))
    pl.loop(0, ROUNDS - EARLY)(functools.partial(finish, (row_round, go_round)))
    pl.loop(0, ROUNDS - LATE)(functools.partial(finish, (back_round, home_round)))
    pl.loop(0, PER * LATE)(functools.partial(finish, (back_fine, home_fine)))


def last_kernel(h_ref, a_ref, w_ref, out, sem):
    def store(n):
        rows = chunk(n, BLOCK)
        return pltpu.make_async_copy(out.at[rows], w_ref.at[rows], sem.at[n])

    @pl.loop(0, BLOCKS)
    def _(n):
        rows = chunk(n, BLOCK)
        out[rows, :] = dot(h_ref[rows, :], a_ref[...], 1, 0)
        store(n).start()

    @pl.loop(0, BLOCKS)
    def _(n):
        store(n).wait()


def solution(mesh):
    def local_apply(field_u, fac_a, fac_b, fac_c, diag_d):
        batch = field_u.shape[0]
        any_space = pl.BlockSpec(memory_space=pl.ANY)
        vmem = pl.BlockSpec(memory_space=pltpu.VMEM)

        def in_hbm(array):
            return pltpu.with_memory_space_constraint(array, pltpu.HBM)

        operands = (jnp.transpose(field_u, (0, 2, 3, 1)), fac_a, fac_b, fac_c, diag_d.reshape(S * S, N))
        counts = (ROUNDS - EARLY, PER * EARLY) * 2 + (ROUNDS - LATE, PER * LATE) * 2
        pairs = [pltpu.SemaphoreType.DMA((n, 4)) for n in counts for _ in range(2)]
        h5, last_a = pl.pallas_call(
            exchange_kernel,
            out_shape=(pltpu.VMEM((batch, S, S, N), BF16), pltpu.VMEM((N, N), BF16)),
            in_specs=[any_space] * 5,
            out_specs=(any_space, any_space),
            scratch_shapes=[
                pltpu.VMEM((PER * EARLY, N, FINE, N), BF16),
                pltpu.VMEM((ROUNDS - EARLY, N, S, N), BF16),
                pltpu.VMEM((ROUNDS, 4, S, S, N), BF16),
                pltpu.VMEM((ROUNDS - LATE, N, S, N), BF16),
                pltpu.VMEM((PER * LATE, N, FINE, N), BF16),
                pltpu.VMEM((N * H, N), F32),
                pltpu.VMEM((N * H, N), F32),
                pltpu.VMEM((N * S, N), F32),
                pltpu.VMEM((S, N, N), F32),
                pltpu.VMEM((N, N), BF16),
                pltpu.VMEM((N, N), BF16),
                pltpu.VMEM((N, N), BF16),
                pltpu.VMEM((N, N), BF16),
                pltpu.VMEM((N, N), BF16),
                pltpu.SemaphoreType.DMA((4,)),
                pltpu.SemaphoreType.DMA((4,)),
                pltpu.SemaphoreType.DMA((4,)),
                *pairs,
            ],
            compiler_params=pltpu.CompilerParams(
                collective_id=0, has_side_effects=True, vmem_limit_bytes=44 * 2**20
            ),
            name="exchange",
        )(*(in_hbm(operand) for operand in operands))
        w = pl.pallas_call(
            last_kernel,
            out_shape=jax.ShapeDtypeStruct((BLOCKS * BLOCK, N), F32),
            in_specs=[vmem, vmem],
            out_specs=any_space,
            scratch_shapes=[pltpu.VMEM((BLOCKS * BLOCK, N), F32), pltpu.SemaphoreType.DMA((BLOCKS,))],
            compiler_params=pltpu.CompilerParams(vmem_limit_bytes=24 * 2**20),
            name="last",
        )(h5.reshape(BLOCKS * BLOCK, N), last_a)
        return jnp.transpose(w.reshape(batch, S, S, N), (0, 3, 1, 2))

    spec_field = P("fields", None, "row", "col")
    spec_factor = P("fields", None)
    return jax.shard_map(
        local_apply,
        mesh=mesh,
        in_specs=(spec_field, spec_factor, spec_factor, spec_factor, P(("fields", "row"), "col", None)),
        out_specs=spec_field,
        check_vma=False,
    )
```

```python
import functools

import jax
import jax.numpy as jnp
from jax import lax
from jax.experimental import pallas as pl
from jax.experimental.pallas import tpu as pltpu
from jax.sharding import PartitionSpec as P

MESH = pl.DeviceIdType.MESH
N = 128
S = 32
H = 16
FINE = 8
PER = S // FINE
ROUNDS = 8
EARLY = 1
LATE = 1
GROUP = 4
BLOCKS, BLOCK = 16, 2048
F32, BF16 = jnp.float32, jnp.bfloat16
PEERS = (1, 2, 3)


def xor(value, bits):
    if bits == 0:
        return value
    if bits == 1:
        return value + 1 - 2 * lax.rem(value, 2)
    if bits == 2:
        return lax.rem(value + 2, 4)
    return 3 - value


def chunk(index, size=S):
    return pl.ds(pl.multiple_of(index * size, size), size)


def dot(lhs, rhs, lhs_dim, rhs_dim):
    return lax.dot_general(lhs, rhs, (((lhs_dim,), (rhs_dim,)), ((), ())), preferred_element_type=F32)


def exchange_kernel(
    u_ref, a_hbm, b_hbm, c_hbm, d_ref, o_ref, a_out,
    fine_in, tens, cols, rets, fine_out, front, rear, diag, diag_t,
    a_ref, b_ref, c_ref, b_t, c_t, factor_sem, d_send, d_recv, *sems,
):
    row, col = lax.axis_index("row"), lax.axis_index("col")

    def row_peer(dr):
        return {"row": xor(row, dr), "col": col} if dr else None

    def col_peer(dc):
        return {"row": row, "col": xor(col, dc)} if dc else None

    def copy(src, dst, send, recv, peer):
        if not peer:
            return pltpu.make_async_copy(src, dst, recv)
        return pltpu.make_async_remote_copy(
            src_ref=src, dst_ref=dst, send_sem=send, recv_sem=recv, device_id=peer, device_id_type=MESH
        )

    def paired(which, index, offset):
        return sems[2 * which].at[index, offset], sems[2 * which + 1].at[index, offset]

    def row_round(t, dr):
        src = u_ref.at[(t + EARLY) * 4 + xor(row, dr)]
        return copy(src, tens.at[t, chunk(row)], *paired(0, t, dr), row_peer(dr))

    def row_fine(unit, dr):
        t, z = lax.div(unit, PER), lax.rem(unit, PER)
        src = u_ref.at[t * 4 + xor(row, dr), :, chunk(z, FINE), :]
        return copy(src, fine_in.at[unit, chunk(row)], *paired(1, unit, dr), row_peer(dr))

    def go_round(t, dc):
        dst = cols.at[t + EARLY, col]
        return copy(tens.at[t, chunk(xor(col, dc))], dst, *paired(2, t, dc), col_peer(dc))

    def go_fine(unit, dc):
        t, z = lax.div(unit, PER), lax.rem(unit, PER)
        dst = cols.at[t, col, :, chunk(z, FINE), :]
        return copy(fine_in.at[unit, chunk(xor(col, dc))], dst, *paired(3, unit, dc), col_peer(dc))

    def back_round(t, dc):
        src = cols.at[t, xor(col, dc)]
        return copy(src, rets.at[t, chunk(col)], *paired(4, t, dc), col_peer(dc))

    def back_fine(unit, dc):
        t, z = lax.div(unit, PER) + ROUNDS - LATE, lax.rem(unit, PER)
        src = cols.at[t, xor(col, dc), :, chunk(z, FINE), :]
        return copy(src, fine_out.at[unit, chunk(col)], *paired(5, unit, dc), col_peer(dc))

    def home_round(t, dr):
        dst = o_ref.at[t * 4 + row]
        return copy(rets.at[t, chunk(xor(row, dr))], dst, *paired(6, t, dr), row_peer(dr))

    def home_fine(unit, dr):
        t, z = lax.div(unit, PER) + ROUNDS - LATE, lax.rem(unit, PER)
        dst = o_ref.at[t * 4 + row, :, chunk(z, FINE), :]
        return copy(fine_out.at[unit, chunk(xor(row, dr))], dst, *paired(7, unit, dr), row_peer(dr))

    def start(kind, index):
        for peer in (0, 3, 2, 1) if kind in (row_round, row_fine, home_round, home_fine) else (1, 2, 3, 0):
            kind(index, peer).start()

    def arrive(kind, index):
        kind(index, 0).wait()
        for peer in PEERS:
            kind(index, peer).wait_recv()

    barrier = pltpu.get_barrier_semaphore()
    for peer in PEERS:
        pl.semaphore_signal(barrier, inc=1, device_id=row_peer(peer), device_id_type=MESH)
        pl.semaphore_signal(barrier, inc=1, device_id=col_peer(peer), device_id_type=MESH)
    pl.semaphore_wait(barrier, 2 * len(PEERS))

    @pl.loop(0, PER * EARLY)
    def _(unit):
        start(row_fine, unit)

    start(row_round, 0)

    own_d, far_d = diag.at[chunk(row, S * S)], diag.at[chunk(xor(row, 2), S * S)]
    keep_d = copy(d_ref, own_d, None, d_recv.at[0], None)
    cross_d = copy(d_ref, own_d, d_send.at[1], d_recv.at[1], row_peer(2))
    near_d = copy(d_ref, own_d, d_send.at[2], d_recv.at[2], row_peer(1))
    pass_d = copy(far_d, far_d, d_send.at[3], d_recv.at[3], row_peer(1))
    for start_d in (cross_d, near_d, keep_d):
        start_d.start()

    @pl.loop(1, ROUNDS - EARLY)
    def _(t):
        start(row_round, t)

    factors = [
        pltpu.make_async_copy(a_hbm, a_ref, factor_sem.at[0]),
        pltpu.make_async_copy(b_hbm, b_ref, factor_sem.at[1]),
        pltpu.make_async_copy(c_hbm, c_ref, factor_sem.at[2]),
        pltpu.make_async_copy(a_hbm, a_out, factor_sem.at[3]),
    ]
    for factor in factors:
        factor.start()
    for factor in factors:
        factor.wait()
    b_t[...] = b_ref[...].T
    c_t[...] = c_ref[...].T

    def swapped(matrix, height):
        @pl.loop(0, height // GROUP)
        def _(step):
            lines = [pl.ds(step * GROUP + n, N, stride=height) for n in range(GROUP)]
            side = jnp.concatenate([front[line, :].astype(BF16) for line in lines], axis=1)
            both = dot(matrix[...], side, 1, 0)
            for n, line in enumerate(lines):
                rear[line, :] = both[:, n * N:(n + 1) * N]

    def first_two(view, height):
        @pl.loop(0, 4)
        def _(q):
            block = view[chunk(q)].reshape(S * height, N)
            front[chunk(q, S * height), :] = dot(block, a_ref[...], 1, 1)

        swapped(b_ref, height)

    def fifth(view, height):
        @pl.loop(0, 4)
        def _(q):
            front[chunk(q, S * height), :] = view[chunk(q)].reshape(S * height, N).astype(F32)

        swapped(b_t, height)

    def rounded(view, height):
        @pl.loop(0, 4)
        def _(q):
            view[chunk(q)] = rear[chunk(q, S * height), :].reshape(S, height, N).astype(BF16)

    def fine(here, there, buffer, work, unit):
        arrive(here, unit)
        work(buffer.at[unit], FINE)
        rounded(buffer.at[unit], FINE)
        start(there, unit)

    def whole(here, there, buffer, work, t):
        if here:
            arrive(here, t)

        @pl.loop(0, S // H)
        def _(half):
            view = buffer.at[t, :, chunk(half, H), :]
            work(view, H)
            rounded(view, H)

        start(there, t)

    def middle(t, early):
        if early:
            for n in range(PER):
                arrive(go_fine, PER * t + n)
        else:
            arrive(go_round, t - EARLY)

        @pl.loop(0, S // GROUP)
        def _(step):
            def slab(j):
                return jnp.concatenate([cols[t, c, j] for c in range(4)], axis=0)

            js = [step * GROUP + n for n in range(GROUP)]
            h2 = jnp.concatenate([slab(j) for j in js], axis=1)
            scale = jnp.concatenate([diag_t[j] for j in js], axis=1)
            h3 = (dot(c_ref[...], h2, 1, 0) * scale).astype(BF16)
            h4 = dot(c_t[...], h3, 1, 0).astype(BF16)
            for n, j in enumerate(js):
                for c in range(4):
                    cols[t, c, j] = h4[c * S:(c + 1) * S, n * N:(n + 1) * N]

    def send_back(t, late):
        if late:
            for n in range(PER):
                start(back_fine, PER * (t - ROUNDS + LATE) + n)
        else:
            start(back_round, t)

    first_round = functools.partial(whole, row_round, go_round, tens, first_two)
    fifth_round = functools.partial(whole, None, home_round, rets, fifth)

    pl.loop(0, PER * EARLY)(functools.partial(fine, row_fine, go_fine, fine_in, first_two))
    pl.loop(0, 1)(first_round)
    cross_d.wait_recv()
    pass_d.start()
    keep_d.wait()
    near_d.wait_recv()
    pass_d.wait_recv()

    @pl.loop(0, S)
    def _(j):
        diag_t[j] = diag[pl.ds(j, N, stride=S), :].T

    pl.loop(1, ROUNDS - EARLY)(first_round)
    at_end = lax.rem(col, 3) == 0

    def body(t, early=False, late=False, fifths=True):
        middle(t, early)
        if not fifths:
            send_back(t, late)
            return

        @pl.when(jnp.logical_not(at_end))
        def _():
            send_back(t, late)

        arrive(back_round, t - 1)

        @pl.when(at_end)
        def _():
            send_back(t, late)

        fifth_round(t - 1)

    pl.loop(0, 1)(functools.partial(body, early=True, fifths=False))
    pl.loop(1, ROUNDS - LATE)(body)
    pl.loop(ROUNDS - LATE, ROUNDS)(functools.partial(body, late=True))
    pl.loop(0, PER * LATE)(functools.partial(fine, back_fine, home_fine, fine_out, fifth))

    def finish(kinds, index):
        for kind in kinds:
            if kind in (home_round, home_fine):
                arrive(kind, index)
            for peer in PEERS:
                kind(index, peer).wait_send()

    for sent in (cross_d, near_d, pass_d):
        sent.wait_send()
    pl.loop(0, PER * EARLY)(functools.partial(finish, (row_fine, go_fine)))
    pl.loop(0, ROUNDS - EARLY)(functools.partial(finish, (row_round, go_round)))
    pl.loop(0, ROUNDS - LATE)(functools.partial(finish, (back_round, home_round)))
    pl.loop(0, PER * LATE)(functools.partial(finish, (back_fine, home_fine)))


def last_kernel(h_ref, a_ref, w_ref, out, sem):
    def store(n):
        rows = chunk(n, BLOCK)
        return pltpu.make_async_copy(out.at[rows], w_ref.at[rows], sem.at[n])

    @pl.loop(0, BLOCKS)
    def _(n):
        rows = chunk(n, BLOCK)
        out[rows, :] = dot(h_ref[rows, :], a_ref[...], 1, 0)
        store(n).start()

    @pl.loop(0, BLOCKS)
    def _(n):
        store(n).wait()


def solution(mesh):
    def local_apply(field_u, fac_a, fac_b, fac_c, diag_d):
        batch = field_u.shape[0]
        any_space = pl.BlockSpec(memory_space=pl.ANY)
        vmem = pl.BlockSpec(memory_space=pltpu.VMEM)

        def in_hbm(array):
            return pltpu.with_memory_space_constraint(array, pltpu.HBM)

        operands = (jnp.transpose(field_u, (0, 2, 3, 1)), fac_a, fac_b, fac_c, diag_d.reshape(S * S, N))
        counts = (ROUNDS - EARLY, PER * EARLY) * 2 + (ROUNDS - LATE, PER * LATE) * 2
        pairs = [pltpu.SemaphoreType.DMA((n, 4)) for n in counts for _ in range(2)]
        h5, last_a = pl.pallas_call(
            exchange_kernel,
            out_shape=(pltpu.VMEM((batch, S, S, N), BF16), pltpu.VMEM((N, N), BF16)),
            in_specs=[any_space] * 5,
            out_specs=(any_space, any_space),
            scratch_shapes=[
                pltpu.VMEM((PER * EARLY, N, FINE, N), BF16),
                pltpu.VMEM((ROUNDS - EARLY, N, S, N), BF16),
                pltpu.VMEM((ROUNDS, 4, S, S, N), BF16),
                pltpu.VMEM((ROUNDS - LATE, N, S, N), BF16),
                pltpu.VMEM((PER * LATE, N, FINE, N), BF16),
                pltpu.VMEM((N * H, N), F32),
                pltpu.VMEM((N * H, N), F32),
                pltpu.VMEM((N * S, N), F32),
                pltpu.VMEM((S, N, N), F32),
                pltpu.VMEM((N, N), BF16),
                pltpu.VMEM((N, N), BF16),
                pltpu.VMEM((N, N), BF16),
                pltpu.VMEM((N, N), BF16),
                pltpu.VMEM((N, N), BF16),
                pltpu.SemaphoreType.DMA((4,)),
                pltpu.SemaphoreType.DMA((4,)),
                pltpu.SemaphoreType.DMA((4,)),
                *pairs,
            ],
            compiler_params=pltpu.CompilerParams(
                collective_id=0, has_side_effects=True, vmem_limit_bytes=44 * 2**20
            ),
            name="exchange",
        )(*(in_hbm(operand) for operand in operands))
        w = pl.pallas_call(
            last_kernel,
            out_shape=jax.ShapeDtypeStruct((BLOCKS * BLOCK, N), F32),
            in_specs=[vmem, vmem],
            out_specs=any_space,
            scratch_shapes=[pltpu.VMEM((BLOCKS * BLOCK, N), F32), pltpu.SemaphoreType.DMA((BLOCKS,))],
            compiler_params=pltpu.CompilerParams(vmem_limit_bytes=24 * 2**20),
            name="last",
        )(h5.reshape(BLOCKS * BLOCK, N), last_a)
        return jnp.transpose(w.reshape(batch, S, S, N), (0, 3, 1, 2))

    spec_field = P("fields", None, "row", "col")
    spec_factor = P("fields", None)
    return jax.shard_map(
        local_apply,
        mesh=mesh,
        in_specs=(spec_field, spec_factor, spec_factor, spec_factor, P(("fields", "row"), "col", None)),
        out_specs=spec_field,
        check_vma=False,
    )
```

```python
import functools

import jax
import jax.numpy as jnp
from jax import lax
from jax.experimental import pallas as pl
from jax.experimental.pallas import tpu as pltpu
from jax.sharding import PartitionSpec as P

MESH = pl.DeviceIdType.MESH
N = 128
S = 32
H = 16
FINE = 8
PER = S // FINE
ROUNDS = 8
EARLY = 1
LATE = 1
GROUP = 4
BLOCKS, BLOCK = 16, 2048
F32, BF16 = jnp.float32, jnp.bfloat16
PEERS = (1, 2, 3)


def xor(value, bits):
    if bits == 0:
        return value
    if bits == 1:
        return value + 1 - 2 * lax.rem(value, 2)
    if bits == 2:
        return lax.rem(value + 2, 4)
    return 3 - value


def chunk(index, size=S):
    return pl.ds(pl.multiple_of(index * size, size), size)


def dot(lhs, rhs, lhs_dim, rhs_dim):
    return lax.dot_general(lhs, rhs, (((lhs_dim,), (rhs_dim,)), ((), ())), preferred_element_type=F32)


def exchange_kernel(
    u_ref, a_hbm, b_hbm, c_hbm, d_ref, o_ref, a_out,
    fine_in, tens, cols, rets, fine_out, front, rear, diag, diag_t,
    a_ref, b_ref, c_ref, b_t, c_t, factor_sem, d_send, d_recv, *sems,
):
    row, col = lax.axis_index("row"), lax.axis_index("col")

    def row_peer(dr):
        return {"row": xor(row, dr), "col": col} if dr else None

    def col_peer(dc):
        return {"row": row, "col": xor(col, dc)} if dc else None

    def copy(src, dst, send, recv, peer):
        if not peer:
            return pltpu.make_async_copy(src, dst, recv)
        return pltpu.make_async_remote_copy(
            src_ref=src, dst_ref=dst, send_sem=send, recv_sem=recv, device_id=peer, device_id_type=MESH
        )

    def paired(which, index, offset):
        return sems[2 * which].at[index, offset], sems[2 * which + 1].at[index, offset]

    def row_round(t, dr):
        src = u_ref.at[(t + EARLY) * 4 + xor(row, dr)]
        return copy(src, tens.at[t, chunk(row)], *paired(0, t, dr), row_peer(dr))

    def row_fine(unit, dr):
        t, z = lax.div(unit, PER), lax.rem(unit, PER)
        src = u_ref.at[t * 4 + xor(row, dr), :, chunk(z, FINE), :]
        return copy(src, fine_in.at[unit, chunk(row)], *paired(1, unit, dr), row_peer(dr))

    def go_round(t, dc):
        dst = cols.at[t + EARLY, col]
        return copy(tens.at[t, chunk(xor(col, dc))], dst, *paired(2, t, dc), col_peer(dc))

    def go_fine(unit, dc):
        t, z = lax.div(unit, PER), lax.rem(unit, PER)
        dst = cols.at[t, col, :, chunk(z, FINE), :]
        return copy(fine_in.at[unit, chunk(xor(col, dc))], dst, *paired(3, unit, dc), col_peer(dc))

    def back_round(t, dc):
        src = cols.at[t, xor(col, dc)]
        return copy(src, rets.at[t, chunk(col)], *paired(4, t, dc), col_peer(dc))

    def back_fine(unit, dc):
        t, z = lax.div(unit, PER) + ROUNDS - LATE, lax.rem(unit, PER)
        src = cols.at[t, xor(col, dc), :, chunk(z, FINE), :]
        return copy(src, fine_out.at[unit, chunk(col)], *paired(5, unit, dc), col_peer(dc))

    def home_round(t, dr):
        dst = o_ref.at[t * 4 + row]
        return copy(rets.at[t, chunk(xor(row, dr))], dst, *paired(6, t, dr), row_peer(dr))

    def home_fine(unit, dr):
        t, z = lax.div(unit, PER) + ROUNDS - LATE, lax.rem(unit, PER)
        dst = o_ref.at[t * 4 + row, :, chunk(z, FINE), :]
        return copy(fine_out.at[unit, chunk(xor(row, dr))], dst, *paired(7, unit, dr), row_peer(dr))

    def start(kind, index):
        for peer in (3, 2, 1, 0) if kind in (row_round, row_fine, home_round, home_fine) else (1, 2, 3, 0):
            kind(index, peer).start()

    def arrive(kind, index):
        kind(index, 0).wait()
        for peer in PEERS:
            kind(index, peer).wait_recv()

    barrier = pltpu.get_barrier_semaphore()
    for peer in PEERS:
        pl.semaphore_signal(barrier, inc=1, device_id=row_peer(peer), device_id_type=MESH)
        pl.semaphore_signal(barrier, inc=1, device_id=col_peer(peer), device_id_type=MESH)
    pl.semaphore_wait(barrier, 2 * len(PEERS))

    for core, order in enumerate(((2, 3, 1, 0), (3, 2, 1, 0))):

        @pl.when(lax.rem(row, 2) == core)
        def _():
            for peer in order:
                row_fine(0, peer).start()

    @pl.loop(1, PER * EARLY)
    def _(unit):
        start(row_fine, unit)

    start(row_round, 0)

    own_d, far_d = diag.at[chunk(row, S * S)], diag.at[chunk(xor(row, 2), S * S)]
    keep_d = copy(d_ref, own_d, None, d_recv.at[0], None)
    cross_d = copy(d_ref, own_d, d_send.at[1], d_recv.at[1], row_peer(2))
    near_d = copy(d_ref, own_d, d_send.at[2], d_recv.at[2], row_peer(1))
    pass_d = copy(far_d, far_d, d_send.at[3], d_recv.at[3], row_peer(1))
    for start_d in (cross_d, near_d, keep_d):
        start_d.start()

    @pl.loop(1, ROUNDS - EARLY)
    def _(t):
        start(row_round, t)

    factors = [
        pltpu.make_async_copy(a_hbm, a_ref, factor_sem.at[0]),
        pltpu.make_async_copy(b_hbm, b_ref, factor_sem.at[1]),
        pltpu.make_async_copy(c_hbm, c_ref, factor_sem.at[2]),
        pltpu.make_async_copy(a_hbm, a_out, factor_sem.at[3]),
    ]
    for factor in factors:
        factor.start()
    for factor in factors:
        factor.wait()
    b_t[...] = b_ref[...].T
    c_t[...] = c_ref[...].T

    def swapped(matrix, height):
        @pl.loop(0, height // GROUP)
        def _(step):
            lines = [pl.ds(step * GROUP + n, N, stride=height) for n in range(GROUP)]
            side = jnp.concatenate([front[line, :].astype(BF16) for line in lines], axis=1)
            both = dot(matrix[...], side, 1, 0)
            for n, line in enumerate(lines):
                rear[line, :] = both[:, n * N:(n + 1) * N]

    def first_two(view, height):
        @pl.loop(0, 4)
        def _(q):
            block = view[chunk(q)].reshape(S * height, N)
            front[chunk(q, S * height), :] = dot(block, a_ref[...], 1, 1)

        swapped(b_ref, height)

    def fifth(view, height):
        @pl.loop(0, 4)
        def _(q):
            front[chunk(q, S * height), :] = view[chunk(q)].reshape(S * height, N).astype(F32)

        swapped(b_t, height)

    def rounded(view, height):
        @pl.loop(0, 4)
        def _(q):
            view[chunk(q)] = rear[chunk(q, S * height), :].reshape(S, height, N).astype(BF16)

    def fine(here, there, buffer, work, unit):
        arrive(here, unit)
        work(buffer.at[unit], FINE)
        rounded(buffer.at[unit], FINE)
        start(there, unit)

    def whole(here, there, buffer, work, t):
        if here:
            arrive(here, t)

        @pl.loop(0, S // H)
        def _(half):
            view = buffer.at[t, :, chunk(half, H), :]
            work(view, H)
            rounded(view, H)

        start(there, t)

    def middle(t, early):
        if early:
            for n in range(PER):
                arrive(go_fine, PER * t + n)
        else:
            arrive(go_round, t - EARLY)

        @pl.loop(0, S // GROUP)
        def _(step):
            def slab(j):
                return jnp.concatenate([cols[t, c, j] for c in range(4)], axis=0)

            js = [step * GROUP + n for n in range(GROUP)]
            h2 = jnp.concatenate([slab(j) for j in js], axis=1)
            scale = jnp.concatenate([diag_t[j] for j in js], axis=1)
            h3 = (dot(c_ref[...], h2, 1, 0) * scale).astype(BF16)
            h4 = dot(c_t[...], h3, 1, 0).astype(BF16)
            for n, j in enumerate(js):
                for c in range(4):
                    cols[t, c, j] = h4[c * S:(c + 1) * S, n * N:(n + 1) * N]

    def send_back(t, late):
        if late:
            for n in range(PER):
                start(back_fine, PER * (t - ROUNDS + LATE) + n)
        else:
            start(back_round, t)

    first_round = functools.partial(whole, row_round, go_round, tens, first_two)
    fifth_round = functools.partial(whole, None, home_round, rets, fifth)

    pl.loop(0, PER * EARLY)(functools.partial(fine, row_fine, go_fine, fine_in, first_two))
    pl.loop(0, 1)(first_round)
    cross_d.wait_recv()
    pass_d.start()
    keep_d.wait()
    near_d.wait_recv()
    pass_d.wait_recv()

    @pl.loop(0, S)
    def _(j):
        diag_t[j] = diag[pl.ds(j, N, stride=S), :].T

    pl.loop(1, ROUNDS - EARLY)(first_round)
    at_end = lax.rem(col, 3) == 0

    def body(t, early=False, late=False, fifths=True):
        middle(t, early)
        if not fifths:
            send_back(t, late)
            return

        @pl.when(jnp.logical_not(at_end))
        def _():
            send_back(t, late)

        arrive(back_round, t - 1)

        @pl.when(at_end)
        def _():
            send_back(t, late)

        fifth_round(t - 1)

    pl.loop(0, 1)(functools.partial(body, early=True, fifths=False))
    pl.loop(1, ROUNDS - LATE)(body)
    pl.loop(ROUNDS - LATE, ROUNDS)(functools.partial(body, late=True))
    pl.loop(0, PER * LATE)(functools.partial(fine, back_fine, home_fine, fine_out, fifth))

    def finish(kinds, index):
        for kind in kinds:
            if kind in (home_round, home_fine):
                arrive(kind, index)
            for peer in PEERS:
                kind(index, peer).wait_send()

    for sent in (cross_d, near_d, pass_d):
        sent.wait_send()
    pl.loop(0, PER * EARLY)(functools.partial(finish, (row_fine, go_fine)))
    pl.loop(0, ROUNDS - EARLY)(functools.partial(finish, (row_round, go_round)))
    pl.loop(0, ROUNDS - LATE)(functools.partial(finish, (back_round, home_round)))
    pl.loop(0, PER * LATE)(functools.partial(finish, (back_fine, home_fine)))


def last_kernel(h_ref, a_ref, w_ref, out, sem):
    def store(n):
        rows = chunk(n, BLOCK)
        return pltpu.make_async_copy(out.at[rows], w_ref.at[rows], sem.at[n])

    @pl.loop(0, BLOCKS)
    def _(n):
        rows = chunk(n, BLOCK)
        out[rows, :] = dot(h_ref[rows, :], a_ref[...], 1, 0)
        store(n).start()

    @pl.loop(0, BLOCKS)
    def _(n):
        store(n).wait()


def solution(mesh):
    def local_apply(field_u, fac_a, fac_b, fac_c, diag_d):
        batch = field_u.shape[0]
        any_space = pl.BlockSpec(memory_space=pl.ANY)
        vmem = pl.BlockSpec(memory_space=pltpu.VMEM)

        def in_hbm(array):
            return pltpu.with_memory_space_constraint(array, pltpu.HBM)

        operands = (jnp.transpose(field_u, (0, 2, 3, 1)), fac_a, fac_b, fac_c, diag_d.reshape(S * S, N))
        counts = (ROUNDS - EARLY, PER * EARLY) * 2 + (ROUNDS - LATE, PER * LATE) * 2
        pairs = [pltpu.SemaphoreType.DMA((n, 4)) for n in counts for _ in range(2)]
        h5, last_a = pl.pallas_call(
            exchange_kernel,
            out_shape=(pltpu.VMEM((batch, S, S, N), BF16), pltpu.VMEM((N, N), BF16)),
            in_specs=[any_space] * 5,
            out_specs=(any_space, any_space),
            scratch_shapes=[
                pltpu.VMEM((PER * EARLY, N, FINE, N), BF16),
                pltpu.VMEM((ROUNDS - EARLY, N, S, N), BF16),
                pltpu.VMEM((ROUNDS, 4, S, S, N), BF16),
                pltpu.VMEM((ROUNDS - LATE, N, S, N), BF16),
                pltpu.VMEM((PER * LATE, N, FINE, N), BF16),
                pltpu.VMEM((N * H, N), F32),
                pltpu.VMEM((N * H, N), F32),
                pltpu.VMEM((N * S, N), F32),
                pltpu.VMEM((S, N, N), F32),
                pltpu.VMEM((N, N), BF16),
                pltpu.VMEM((N, N), BF16),
                pltpu.VMEM((N, N), BF16),
                pltpu.VMEM((N, N), BF16),
                pltpu.VMEM((N, N), BF16),
                pltpu.SemaphoreType.DMA((4,)),
                pltpu.SemaphoreType.DMA((4,)),
                pltpu.SemaphoreType.DMA((4,)),
                *pairs,
            ],
            compiler_params=pltpu.CompilerParams(
                collective_id=0, has_side_effects=True, vmem_limit_bytes=44 * 2**20
            ),
            name="exchange",
        )(*(in_hbm(operand) for operand in operands))
        w = pl.pallas_call(
            last_kernel,
            out_shape=jax.ShapeDtypeStruct((BLOCKS * BLOCK, N), F32),
            in_specs=[vmem, vmem],
            out_specs=any_space,
            scratch_shapes=[pltpu.VMEM((BLOCKS * BLOCK, N), F32), pltpu.SemaphoreType.DMA((BLOCKS,))],
            compiler_params=pltpu.CompilerParams(vmem_limit_bytes=24 * 2**20),
            name="last",
        )(h5.reshape(BLOCKS * BLOCK, N), last_a)
        return jnp.transpose(w.reshape(batch, S, S, N), (0, 3, 1, 2))

    spec_field = P("fields", None, "row", "col")
    spec_factor = P("fields", None)
    return jax.shard_map(
        local_apply,
        mesh=mesh,
        in_specs=(spec_field, spec_factor, spec_factor, spec_factor, P(("fields", "row"), "col", None)),
        out_specs=spec_field,
        check_vma=False,
    )
```

```python
import functools

import jax
import jax.numpy as jnp
from jax import lax
from jax.experimental import pallas as pl
from jax.experimental.pallas import tpu as pltpu
from jax.sharding import PartitionSpec as P

MESH = pl.DeviceIdType.MESH
N = 128
S = 32
H = 16
FINE = 8
PER = S // FINE
ROUNDS = 8
EARLY = 1
LATE = 1
GROUP = 4
BLOCKS, BLOCK = 16, 2048
F32, BF16 = jnp.float32, jnp.bfloat16
PEERS = (1, 2, 3)


def xor(value, bits):
    if bits == 0:
        return value
    if bits == 1:
        return value + 1 - 2 * lax.rem(value, 2)
    if bits == 2:
        return lax.rem(value + 2, 4)
    return 3 - value


def chunk(index, size=S):
    return pl.ds(pl.multiple_of(index * size, size), size)


def dot(lhs, rhs, lhs_dim, rhs_dim):
    return lax.dot_general(lhs, rhs, (((lhs_dim,), (rhs_dim,)), ((), ())), preferred_element_type=F32)


def exchange_kernel(
    u_ref, a_hbm, b_hbm, c_hbm, d_ref, o_ref, a_out,
    fine_in, tens, cols, rets, fine_out, front, rear, diag, diag_t,
    a_ref, b_ref, c_ref, b_t, c_t, factor_sem, d_send, d_recv, *sems,
):
    row, col = lax.axis_index("row"), lax.axis_index("col")

    def row_peer(dr):
        return {"row": xor(row, dr), "col": col} if dr else None

    def col_peer(dc):
        return {"row": row, "col": xor(col, dc)} if dc else None

    def copy(src, dst, send, recv, peer):
        if not peer:
            return pltpu.make_async_copy(src, dst, recv)
        return pltpu.make_async_remote_copy(
            src_ref=src, dst_ref=dst, send_sem=send, recv_sem=recv, device_id=peer, device_id_type=MESH
        )

    def paired(which, index, offset):
        return sems[2 * which].at[index, offset], sems[2 * which + 1].at[index, offset]

    def row_round(t, dr):
        src = u_ref.at[(t + EARLY) * 4 + xor(row, dr)]
        return copy(src, tens.at[t, chunk(row)], *paired(0, t, dr), row_peer(dr))

    def row_fine(unit, dr):
        t, z = lax.div(unit, PER), lax.rem(unit, PER)
        src = u_ref.at[t * 4 + xor(row, dr), :, chunk(z, FINE), :]
        return copy(src, fine_in.at[unit, chunk(row)], *paired(1, unit, dr), row_peer(dr))

    def go_round(t, dc):
        dst = cols.at[t + EARLY, col]
        return copy(tens.at[t, chunk(xor(col, dc))], dst, *paired(2, t, dc), col_peer(dc))

    def go_fine(unit, dc):
        t, z = lax.div(unit, PER), lax.rem(unit, PER)
        dst = cols.at[t, col, :, chunk(z, FINE), :]
        return copy(fine_in.at[unit, chunk(xor(col, dc))], dst, *paired(3, unit, dc), col_peer(dc))

    def back_round(t, dc):
        src = cols.at[t, xor(col, dc)]
        return copy(src, rets.at[t, chunk(col)], *paired(4, t, dc), col_peer(dc))

    def back_fine(unit, dc):
        t, z = lax.div(unit, PER) + ROUNDS - LATE, lax.rem(unit, PER)
        src = cols.at[t, xor(col, dc), :, chunk(z, FINE), :]
        return copy(src, fine_out.at[unit, chunk(col)], *paired(5, unit, dc), col_peer(dc))

    def home_round(t, dr):
        dst = o_ref.at[t * 4 + row]
        return copy(rets.at[t, chunk(xor(row, dr))], dst, *paired(6, t, dr), row_peer(dr))

    def home_fine(unit, dr):
        t, z = lax.div(unit, PER) + ROUNDS - LATE, lax.rem(unit, PER)
        dst = o_ref.at[t * 4 + row, :, chunk(z, FINE), :]
        return copy(fine_out.at[unit, chunk(xor(row, dr))], dst, *paired(7, unit, dr), row_peer(dr))

    def start(kind, index):
        for peer in (0, 3, 2, 1) if kind in (row_round, row_fine, home_round, home_fine) else (3, 2, 1, 0):
            kind(index, peer).start()

    def arrive(kind, index):
        kind(index, 0).wait()
        for peer in PEERS:
            kind(index, peer).wait_recv()

    barrier = pltpu.get_barrier_semaphore()
    for peer in PEERS:
        pl.semaphore_signal(barrier, inc=1, device_id=row_peer(peer), device_id_type=MESH)
        pl.semaphore_signal(barrier, inc=1, device_id=col_peer(peer), device_id_type=MESH)
    pl.semaphore_wait(barrier, 2 * len(PEERS))

    @pl.loop(0, PER * EARLY)
    def _(unit):
        start(row_fine, unit)

    start(row_round, 0)

    own_d, far_d = diag.at[chunk(row, S * S)], diag.at[chunk(xor(row, 2), S * S)]
    keep_d = copy(d_ref, own_d, None, d_recv.at[0], None)
    cross_d = copy(d_ref, own_d, d_send.at[1], d_recv.at[1], row_peer(2))
    near_d = copy(d_ref, own_d, d_send.at[2], d_recv.at[2], row_peer(1))
    pass_d = copy(far_d, far_d, d_send.at[3], d_recv.at[3], row_peer(1))
    for start_d in (cross_d, near_d, keep_d):
        start_d.start()

    @pl.loop(1, ROUNDS - EARLY)
    def _(t):
        start(row_round, t)

    factors = [
        pltpu.make_async_copy(a_hbm, a_ref, factor_sem.at[0]),
        pltpu.make_async_copy(b_hbm, b_ref, factor_sem.at[1]),
        pltpu.make_async_copy(c_hbm, c_ref, factor_sem.at[2]),
        pltpu.make_async_copy(a_hbm, a_out, factor_sem.at[3]),
    ]
    for factor in factors:
        factor.start()
    for factor in factors:
        factor.wait()
    b_t[...] = b_ref[...].T
    c_t[...] = c_ref[...].T

    def swapped(matrix, height):
        @pl.loop(0, height // GROUP)
        def _(step):
            lines = [pl.ds(step * GROUP + n, N, stride=height) for n in range(GROUP)]
            side = jnp.concatenate([front[line, :].astype(BF16) for line in lines], axis=1)
            both = dot(matrix[...], side, 1, 0)
            for n, line in enumerate(lines):
                rear[line, :] = both[:, n * N:(n + 1) * N]

    def first_two(view, height):
        @pl.loop(0, 4)
        def _(q):
            block = view[chunk(q)].reshape(S * height, N)
            front[chunk(q, S * height), :] = dot(block, a_ref[...], 1, 1)

        swapped(b_ref, height)

    def fifth(view, height):
        @pl.loop(0, 4)
        def _(q):
            front[chunk(q, S * height), :] = view[chunk(q)].reshape(S * height, N).astype(F32)

        swapped(b_t, height)

    def rounded(view, height):
        @pl.loop(0, 4)
        def _(q):
            view[chunk(q)] = rear[chunk(q, S * height), :].reshape(S, height, N).astype(BF16)

    def fine(here, there, buffer, work, unit):
        arrive(here, unit)
        work(buffer.at[unit], FINE)
        rounded(buffer.at[unit], FINE)
        start(there, unit)

    def whole(here, there, buffer, work, t):
        if here:
            arrive(here, t)

        @pl.loop(0, S // H)
        def _(half):
            view = buffer.at[t, :, chunk(half, H), :]
            work(view, H)
            rounded(view, H)

        start(there, t)

    def middle(t, early):
        if early:
            for n in range(PER):
                arrive(go_fine, PER * t + n)
        else:
            arrive(go_round, t - EARLY)

        @pl.loop(0, S // GROUP)
        def _(step):
            def slab(j):
                return jnp.concatenate([cols[t, c, j] for c in range(4)], axis=0)

            js = [step * GROUP + n for n in range(GROUP)]
            h2 = jnp.concatenate([slab(j) for j in js], axis=1)
            scale = jnp.concatenate([diag_t[j] for j in js], axis=1)
            h3 = (dot(c_ref[...], h2, 1, 0) * scale).astype(BF16)
            h4 = dot(c_t[...], h3, 1, 0).astype(BF16)
            for n, j in enumerate(js):
                for c in range(4):
                    cols[t, c, j] = h4[c * S:(c + 1) * S, n * N:(n + 1) * N]

    def send_back(t, late):
        if late:
            for n in range(PER):
                start(back_fine, PER * (t - ROUNDS + LATE) + n)
        else:
            start(back_round, t)

    first_round = functools.partial(whole, row_round, go_round, tens, first_two)
    fifth_round = functools.partial(whole, None, home_round, rets, fifth)

    pl.loop(0, PER * EARLY)(functools.partial(fine, row_fine, go_fine, fine_in, first_two))
    pl.loop(0, 1)(first_round)
    cross_d.wait_recv()
    pass_d.start()
    keep_d.wait()
    near_d.wait_recv()
    pass_d.wait_recv()

    @pl.loop(0, S)
    def _(j):
        diag_t[j] = diag[pl.ds(j, N, stride=S), :].T

    pl.loop(1, ROUNDS - EARLY)(first_round)
    at_end = lax.rem(col, 3) == 0

    def body(t, early=False, late=False, fifths=True):
        middle(t, early)
        if not fifths:
            send_back(t, late)
            return

        @pl.when(jnp.logical_not(at_end))
        def _():
            send_back(t, late)

        arrive(back_round, t - 1)

        @pl.when(at_end)
        def _():
            send_back(t, late)

        fifth_round(t - 1)

    pl.loop(0, 1)(functools.partial(body, early=True, fifths=False))
    pl.loop(1, ROUNDS - LATE)(body)
    pl.loop(ROUNDS - LATE, ROUNDS)(functools.partial(body, late=True))
    pl.loop(0, PER * LATE)(functools.partial(fine, back_fine, home_fine, fine_out, fifth))

    def finish(kinds, index):
        for kind in kinds:
            if kind in (home_round, home_fine):
                arrive(kind, index)
            for peer in PEERS:
                kind(index, peer).wait_send()

    for sent in (cross_d, near_d, pass_d):
        sent.wait_send()
    pl.loop(0, PER * EARLY)(functools.partial(finish, (row_fine, go_fine)))
    pl.loop(0, ROUNDS - EARLY)(functools.partial(finish, (row_round, go_round)))
    pl.loop(0, ROUNDS - LATE)(functools.partial(finish, (back_round, home_round)))
    pl.loop(0, PER * LATE)(functools.partial(finish, (back_fine, home_fine)))


def last_kernel(h_ref, a_ref, w_ref, out, sem):
    def store(n):
        rows = chunk(n, BLOCK)
        return pltpu.make_async_copy(out.at[rows], w_ref.at[rows], sem.at[n])

    @pl.loop(0, BLOCKS)
    def _(n):
        rows = chunk(n, BLOCK)
        out[rows, :] = dot(h_ref[rows, :], a_ref[...], 1, 0)
        store(n).start()

    @pl.loop(0, BLOCKS)
    def _(n):
        store(n).wait()


def solution(mesh):
    def local_apply(field_u, fac_a, fac_b, fac_c, diag_d):
        batch = field_u.shape[0]
        any_space = pl.BlockSpec(memory_space=pl.ANY)
        vmem = pl.BlockSpec(memory_space=pltpu.VMEM)

        def in_hbm(array):
            return pltpu.with_memory_space_constraint(array, pltpu.HBM)

        operands = (jnp.transpose(field_u, (0, 2, 3, 1)), fac_a, fac_b, fac_c, diag_d.reshape(S * S, N))
        counts = (ROUNDS - EARLY, PER * EARLY) * 2 + (ROUNDS - LATE, PER * LATE) * 2
        pairs = [pltpu.SemaphoreType.DMA((n, 4)) for n in counts for _ in range(2)]
        h5, last_a = pl.pallas_call(
            exchange_kernel,
            out_shape=(pltpu.VMEM((batch, S, S, N), BF16), pltpu.VMEM((N, N), BF16)),
            in_specs=[any_space] * 5,
            out_specs=(any_space, any_space),
            scratch_shapes=[
                pltpu.VMEM((PER * EARLY, N, FINE, N), BF16),
                pltpu.VMEM((ROUNDS - EARLY, N, S, N), BF16),
                pltpu.VMEM((ROUNDS, 4, S, S, N), BF16),
                pltpu.VMEM((ROUNDS - LATE, N, S, N), BF16),
                pltpu.VMEM((PER * LATE, N, FINE, N), BF16),
                pltpu.VMEM((N * H, N), F32),
                pltpu.VMEM((N * H, N), F32),
                pltpu.VMEM((N * S, N), F32),
                pltpu.VMEM((S, N, N), F32),
                pltpu.VMEM((N, N), BF16),
                pltpu.VMEM((N, N), BF16),
                pltpu.VMEM((N, N), BF16),
                pltpu.VMEM((N, N), BF16),
                pltpu.VMEM((N, N), BF16),
                pltpu.SemaphoreType.DMA((4,)),
                pltpu.SemaphoreType.DMA((4,)),
                pltpu.SemaphoreType.DMA((4,)),
                *pairs,
            ],
            compiler_params=pltpu.CompilerParams(
                collective_id=0, has_side_effects=True, vmem_limit_bytes=44 * 2**20
            ),
            name="exchange",
        )(*(in_hbm(operand) for operand in operands))
        w = pl.pallas_call(
            last_kernel,
            out_shape=jax.ShapeDtypeStruct((BLOCKS * BLOCK, N), F32),
            in_specs=[vmem, vmem],
            out_specs=any_space,
            scratch_shapes=[pltpu.VMEM((BLOCKS * BLOCK, N), F32), pltpu.SemaphoreType.DMA((BLOCKS,))],
            compiler_params=pltpu.CompilerParams(vmem_limit_bytes=24 * 2**20),
            name="last",
        )(h5.reshape(BLOCKS * BLOCK, N), last_a)
        return jnp.transpose(w.reshape(batch, S, S, N), (0, 3, 1, 2))

    spec_field = P("fields", None, "row", "col")
    spec_factor = P("fields", None)
    return jax.shard_map(
        local_apply,
        mesh=mesh,
        in_specs=(spec_field, spec_factor, spec_factor, spec_factor, P(("fields", "row"), "col", None)),
        out_specs=spec_field,
        check_vma=False,
    )
```

```python
import functools

import jax
import jax.numpy as jnp
from jax import lax
from jax.experimental import pallas as pl
from jax.experimental.pallas import tpu as pltpu
from jax.sharding import PartitionSpec as P

MESH = pl.DeviceIdType.MESH
N = 128
S = 32
H = 16
FINE = 8
PER = S // FINE
ROUNDS = 8
EARLY = 1
LATE = 1
GROUP = 4
BLOCKS, BLOCK = 16, 2048
F32, BF16 = jnp.float32, jnp.bfloat16
PEERS = (1, 2, 3)


def xor(value, bits):
    if bits == 0:
        return value
    if bits == 1:
        return value + 1 - 2 * lax.rem(value, 2)
    if bits == 2:
        return lax.rem(value + 2, 4)
    return 3 - value


def chunk(index, size=S):
    return pl.ds(pl.multiple_of(index * size, size), size)


def dot(lhs, rhs, lhs_dim, rhs_dim):
    return lax.dot_general(lhs, rhs, (((lhs_dim,), (rhs_dim,)), ((), ())), preferred_element_type=F32)


def exchange_kernel(
    u_ref, a_hbm, b_hbm, c_hbm, d_ref, o_ref, a_out,
    fine_in, tens, cols, rets, fine_out, front, rear, diag, diag_t,
    a_ref, b_ref, c_ref, b_t, c_t, factor_sem, d_send, d_recv, *sems,
):
    row, col = lax.axis_index("row"), lax.axis_index("col")

    def row_peer(dr):
        return {"row": xor(row, dr), "col": col} if dr else None

    def col_peer(dc):
        return {"row": row, "col": xor(col, dc)} if dc else None

    def copy(src, dst, send, recv, peer):
        if not peer:
            return pltpu.make_async_copy(src, dst, recv)
        return pltpu.make_async_remote_copy(
            src_ref=src, dst_ref=dst, send_sem=send, recv_sem=recv, device_id=peer, device_id_type=MESH
        )

    def paired(which, index, offset):
        return sems[2 * which].at[index, offset], sems[2 * which + 1].at[index, offset]

    def row_round(t, dr):
        src = u_ref.at[(t + EARLY) * 4 + xor(row, dr)]
        return copy(src, tens.at[t, chunk(row)], *paired(0, t, dr), row_peer(dr))

    def row_fine(unit, dr):
        t, z = lax.div(unit, PER), lax.rem(unit, PER)
        src = u_ref.at[t * 4 + xor(row, dr), :, chunk(z, FINE), :]
        return copy(src, fine_in.at[unit, chunk(row)], *paired(1, unit, dr), row_peer(dr))

    def go_round(t, dc):
        dst = cols.at[t + EARLY, col]
        return copy(tens.at[t, chunk(xor(col, dc))], dst, *paired(2, t, dc), col_peer(dc))

    def go_fine(unit, dc):
        t, z = lax.div(unit, PER), lax.rem(unit, PER)
        dst = cols.at[t, col, :, chunk(z, FINE), :]
        return copy(fine_in.at[unit, chunk(xor(col, dc))], dst, *paired(3, unit, dc), col_peer(dc))

    def back_round(t, dc):
        src = cols.at[t, xor(col, dc)]
        return copy(src, rets.at[t, chunk(col)], *paired(4, t, dc), col_peer(dc))

    def back_fine(unit, dc):
        t, z = lax.div(unit, PER) + ROUNDS - LATE, lax.rem(unit, PER)
        src = cols.at[t, xor(col, dc), :, chunk(z, FINE), :]
        return copy(src, fine_out.at[unit, chunk(col)], *paired(5, unit, dc), col_peer(dc))

    def home_round(t, dr):
        dst = o_ref.at[t * 4 + row]
        return copy(rets.at[t, chunk(xor(row, dr))], dst, *paired(6, t, dr), row_peer(dr))

    def home_fine(unit, dr):
        t, z = lax.div(unit, PER) + ROUNDS - LATE, lax.rem(unit, PER)
        dst = o_ref.at[t * 4 + row, :, chunk(z, FINE), :]
        return copy(fine_out.at[unit, chunk(xor(row, dr))], dst, *paired(7, unit, dr), row_peer(dr))

    def start(kind, index):
        for peer in (0, 3, 2, 1) if kind in (row_round, row_fine, home_round, home_fine) else (2, 3, 1, 0):
            kind(index, peer).start()

    def arrive(kind, index):
        kind(index, 0).wait()
        for peer in PEERS:
            kind(index, peer).wait_recv()

    barrier = pltpu.get_barrier_semaphore()
    for peer in PEERS:
        pl.semaphore_signal(barrier, inc=1, device_id=row_peer(peer), device_id_type=MESH)
        pl.semaphore_signal(barrier, inc=1, device_id=col_peer(peer), device_id_type=MESH)
    pl.semaphore_wait(barrier, 2 * len(PEERS))

    @pl.loop(0, PER * EARLY)
    def _(unit):
        start(row_fine, unit)

    start(row_round, 0)

    own_d, far_d = diag.at[chunk(row, S * S)], diag.at[chunk(xor(row, 2), S * S)]
    keep_d = copy(d_ref, own_d, None, d_recv.at[0], None)
    cross_d = copy(d_ref, own_d, d_send.at[1], d_recv.at[1], row_peer(2))
    near_d = copy(d_ref, own_d, d_send.at[2], d_recv.at[2], row_peer(1))
    pass_d = copy(far_d, far_d, d_send.at[3], d_recv.at[3], row_peer(1))
    for start_d in (cross_d, near_d, keep_d):
        start_d.start()

    @pl.loop(1, ROUNDS - EARLY)
    def _(t):
        start(row_round, t)

    factors = [
        pltpu.make_async_copy(a_hbm, a_ref, factor_sem.at[0]),
        pltpu.make_async_copy(b_hbm, b_ref, factor_sem.at[1]),
        pltpu.make_async_copy(c_hbm, c_ref, factor_sem.at[2]),
        pltpu.make_async_copy(a_hbm, a_out, factor_sem.at[3]),
    ]
    for factor in factors:
        factor.start()
    for factor in factors:
        factor.wait()
    b_t[...] = b_ref[...].T
    c_t[...] = c_ref[...].T

    def swapped(matrix, height):
        @pl.loop(0, height // GROUP)
        def _(step):
            lines = [pl.ds(step * GROUP + n, N, stride=height) for n in range(GROUP)]
            side = jnp.concatenate([front[line, :].astype(BF16) for line in lines], axis=1)
            both = dot(matrix[...], side, 1, 0)
            for n, line in enumerate(lines):
                rear[line, :] = both[:, n * N:(n + 1) * N]

    def first_two(view, height):
        @pl.loop(0, 4)
        def _(q):
            block = view[chunk(q)].reshape(S * height, N)
            front[chunk(q, S * height), :] = dot(block, a_ref[...], 1, 1)

        swapped(b_ref, height)

    def fifth(view, height):
        @pl.loop(0, 4)
        def _(q):
            front[chunk(q, S * height), :] = view[chunk(q)].reshape(S * height, N).astype(F32)

        swapped(b_t, height)

    def rounded(view, height):
        @pl.loop(0, 4)
        def _(q):
            view[chunk(q)] = rear[chunk(q, S * height), :].reshape(S, height, N).astype(BF16)

    def fine(here, there, buffer, work, unit):
        arrive(here, unit)
        work(buffer.at[unit], FINE)
        rounded(buffer.at[unit], FINE)
        start(there, unit)

    def whole(here, there, buffer, work, t):
        if here:
            arrive(here, t)

        @pl.loop(0, S // H)
        def _(half):
            view = buffer.at[t, :, chunk(half, H), :]
            work(view, H)
            rounded(view, H)

        start(there, t)

    def middle(t, early):
        if early:
            for n in range(PER):
                arrive(go_fine, PER * t + n)
        else:
            arrive(go_round, t - EARLY)

        @pl.loop(0, S // GROUP)
        def _(step):
            def slab(j):
                return jnp.concatenate([cols[t, c, j] for c in range(4)], axis=0)

            js = [step * GROUP + n for n in range(GROUP)]
            h2 = jnp.concatenate([slab(j) for j in js], axis=1)
            scale = jnp.concatenate([diag_t[j] for j in js], axis=1)
            h3 = (dot(c_ref[...], h2, 1, 0) * scale).astype(BF16)
            h4 = dot(c_t[...], h3, 1, 0).astype(BF16)
            for n, j in enumerate(js):
                for c in range(4):
                    cols[t, c, j] = h4[c * S:(c + 1) * S, n * N:(n + 1) * N]

    def send_back(t, late):
        if late:
            for n in range(PER):
                start(back_fine, PER * (t - ROUNDS + LATE) + n)
        else:
            start(back_round, t)

    first_round = functools.partial(whole, row_round, go_round, tens, first_two)
    fifth_round = functools.partial(whole, None, home_round, rets, fifth)

    pl.loop(0, PER * EARLY)(functools.partial(fine, row_fine, go_fine, fine_in, first_two))
    pl.loop(0, 1)(first_round)
    cross_d.wait_recv()
    pass_d.start()
    keep_d.wait()
    near_d.wait_recv()
    pass_d.wait_recv()

    @pl.loop(0, S)
    def _(j):
        diag_t[j] = diag[pl.ds(j, N, stride=S), :].T

    pl.loop(1, ROUNDS - EARLY)(first_round)
    at_end = lax.rem(col, 3) == 0

    def body(t, early=False, late=False, fifths=True):
        middle(t, early)
        if not fifths:
            send_back(t, late)
            return

        @pl.when(jnp.logical_not(at_end))
        def _():
            send_back(t, late)

        arrive(back_round, t - 1)

        @pl.when(at_end)
        def _():
            send_back(t, late)

        fifth_round(t - 1)

    pl.loop(0, 1)(functools.partial(body, early=True, fifths=False))
    pl.loop(1, ROUNDS - LATE)(body)
    pl.loop(ROUNDS - LATE, ROUNDS)(functools.partial(body, late=True))
    pl.loop(0, PER * LATE)(functools.partial(fine, back_fine, home_fine, fine_out, fifth))

    def finish(kinds, index):
        for kind in kinds:
            if kind in (home_round, home_fine):
                arrive(kind, index)
            for peer in PEERS:
                kind(index, peer).wait_send()

    for sent in (cross_d, near_d, pass_d):
        sent.wait_send()
    pl.loop(0, PER * EARLY)(functools.partial(finish, (row_fine, go_fine)))
    pl.loop(0, ROUNDS - EARLY)(functools.partial(finish, (row_round, go_round)))
    pl.loop(0, ROUNDS - LATE)(functools.partial(finish, (back_round, home_round)))
    pl.loop(0, PER * LATE)(functools.partial(finish, (back_fine, home_fine)))


def last_kernel(h_ref, a_ref, w_ref, out, sem):
    def store(n):
        rows = chunk(n, BLOCK)
        return pltpu.make_async_copy(out.at[rows], w_ref.at[rows], sem.at[n])

    @pl.loop(0, BLOCKS)
    def _(n):
        rows = chunk(n, BLOCK)
        out[rows, :] = dot(h_ref[rows, :], a_ref[...], 1, 0)
        store(n).start()

    @pl.loop(0, BLOCKS)
    def _(n):
        store(n).wait()


def solution(mesh):
    def local_apply(field_u, fac_a, fac_b, fac_c, diag_d):
        batch = field_u.shape[0]
        any_space = pl.BlockSpec(memory_space=pl.ANY)
        vmem = pl.BlockSpec(memory_space=pltpu.VMEM)

        def in_hbm(array):
            return pltpu.with_memory_space_constraint(array, pltpu.HBM)

        operands = (jnp.transpose(field_u, (0, 2, 3, 1)), fac_a, fac_b, fac_c, diag_d.reshape(S * S, N))
        counts = (ROUNDS - EARLY, PER * EARLY) * 2 + (ROUNDS - LATE, PER * LATE) * 2
        pairs = [pltpu.SemaphoreType.DMA((n, 4)) for n in counts for _ in range(2)]
        h5, last_a = pl.pallas_call(
            exchange_kernel,
            out_shape=(pltpu.VMEM((batch, S, S, N), BF16), pltpu.VMEM((N, N), BF16)),
            in_specs=[any_space] * 5,
            out_specs=(any_space, any_space),
            scratch_shapes=[
                pltpu.VMEM((PER * EARLY, N, FINE, N), BF16),
                pltpu.VMEM((ROUNDS - EARLY, N, S, N), BF16),
                pltpu.VMEM((ROUNDS, 4, S, S, N), BF16),
                pltpu.VMEM((ROUNDS - LATE, N, S, N), BF16),
                pltpu.VMEM((PER * LATE, N, FINE, N), BF16),
                pltpu.VMEM((N * H, N), F32),
                pltpu.VMEM((N * H, N), F32),
                pltpu.VMEM((N * S, N), F32),
                pltpu.VMEM((S, N, N), F32),
                pltpu.VMEM((N, N), BF16),
                pltpu.VMEM((N, N), BF16),
                pltpu.VMEM((N, N), BF16),
                pltpu.VMEM((N, N), BF16),
                pltpu.VMEM((N, N), BF16),
                pltpu.SemaphoreType.DMA((4,)),
                pltpu.SemaphoreType.DMA((4,)),
                pltpu.SemaphoreType.DMA((4,)),
                *pairs,
            ],
            compiler_params=pltpu.CompilerParams(
                collective_id=0, has_side_effects=True, vmem_limit_bytes=44 * 2**20
            ),
            name="exchange",
        )(*(in_hbm(operand) for operand in operands))
        w = pl.pallas_call(
            last_kernel,
            out_shape=jax.ShapeDtypeStruct((BLOCKS * BLOCK, N), F32),
            in_specs=[vmem, vmem],
            out_specs=any_space,
            scratch_shapes=[pltpu.VMEM((BLOCKS * BLOCK, N), F32), pltpu.SemaphoreType.DMA((BLOCKS,))],
            compiler_params=pltpu.CompilerParams(vmem_limit_bytes=24 * 2**20),
            name="last",
        )(h5.reshape(BLOCKS * BLOCK, N), last_a)
        return jnp.transpose(w.reshape(batch, S, S, N), (0, 3, 1, 2))

    spec_field = P("fields", None, "row", "col")
    spec_factor = P("fields", None)
    return jax.shard_map(
        local_apply,
        mesh=mesh,
        in_specs=(spec_field, spec_factor, spec_factor, spec_factor, P(("fields", "row"), "col", None)),
        out_specs=spec_field,
        check_vma=False,
    )
```

```python
import functools

import jax
import jax.numpy as jnp
from jax import lax
from jax.experimental import pallas as pl
from jax.experimental.pallas import tpu as pltpu
from jax.sharding import PartitionSpec as P

MESH = pl.DeviceIdType.MESH
N = 128
S = 32
H = 16
FINE = 8
PER = S // FINE
ROUNDS = 8
EARLY = 1
LATE = 1
GROUP = 4
BLOCKS, BLOCK = 16, 2048
F32, BF16 = jnp.float32, jnp.bfloat16
PEERS = (1, 2, 3)


def xor(value, bits):
    if bits == 0:
        return value
    if bits == 1:
        return value + 1 - 2 * lax.rem(value, 2)
    if bits == 2:
        return lax.rem(value + 2, 4)
    return 3 - value


def chunk(index, size=S):
    return pl.ds(pl.multiple_of(index * size, size), size)


def dot(lhs, rhs, lhs_dim, rhs_dim):
    return lax.dot_general(lhs, rhs, (((lhs_dim,), (rhs_dim,)), ((), ())), preferred_element_type=F32)


def exchange_kernel(
    u_ref, a_hbm, b_hbm, c_hbm, d_ref, o_ref, a_out,
    fine_in, tens, cols, rets, fine_out, front, rear, diag, diag_t,
    a_ref, b_ref, c_ref, b_t, c_t, factor_sem, d_send, d_recv, *sems,
):
    row, col = lax.axis_index("row"), lax.axis_index("col")

    def row_peer(dr):
        return {"row": xor(row, dr), "col": col} if dr else None

    def col_peer(dc):
        return {"row": row, "col": xor(col, dc)} if dc else None

    def copy(src, dst, send, recv, peer):
        if not peer:
            return pltpu.make_async_copy(src, dst, recv)
        return pltpu.make_async_remote_copy(
            src_ref=src, dst_ref=dst, send_sem=send, recv_sem=recv, device_id=peer, device_id_type=MESH
        )

    def paired(which, index, offset):
        return sems[2 * which].at[index, offset], sems[2 * which + 1].at[index, offset]

    def row_round(t, dr):
        src = u_ref.at[(t + EARLY) * 4 + xor(row, dr)]
        return copy(src, tens.at[t, chunk(row)], *paired(0, t, dr), row_peer(dr))

    def row_fine(unit, dr):
        t, z = lax.div(unit, PER), lax.rem(unit, PER)
        src = u_ref.at[t * 4 + xor(row, dr), :, chunk(z, FINE), :]
        return copy(src, fine_in.at[unit, chunk(row)], *paired(1, unit, dr), row_peer(dr))

    def go_round(t, dc):
        dst = cols.at[t + EARLY, col]
        return copy(tens.at[t, chunk(xor(col, dc))], dst, *paired(2, t, dc), col_peer(dc))

    def go_fine(unit, dc):
        t, z = lax.div(unit, PER), lax.rem(unit, PER)
        dst = cols.at[t, col, :, chunk(z, FINE), :]
        return copy(fine_in.at[unit, chunk(xor(col, dc))], dst, *paired(3, unit, dc), col_peer(dc))

    def back_round(t, dc):
        src = cols.at[t, xor(col, dc)]
        return copy(src, rets.at[t, chunk(col)], *paired(4, t, dc), col_peer(dc))

    def back_fine(unit, dc):
        t, z = lax.div(unit, PER) + ROUNDS - LATE, lax.rem(unit, PER)
        src = cols.at[t, xor(col, dc), :, chunk(z, FINE), :]
        return copy(src, fine_out.at[unit, chunk(col)], *paired(5, unit, dc), col_peer(dc))

    def home_round(t, dr):
        dst = o_ref.at[t * 4 + row]
        return copy(rets.at[t, chunk(xor(row, dr))], dst, *paired(6, t, dr), row_peer(dr))

    def home_fine(unit, dr):
        t, z = lax.div(unit, PER) + ROUNDS - LATE, lax.rem(unit, PER)
        dst = o_ref.at[t * 4 + row, :, chunk(z, FINE), :]
        return copy(fine_out.at[unit, chunk(xor(row, dr))], dst, *paired(7, unit, dr), row_peer(dr))

    def start(kind, index):
        for peer in (0, 3, 2, 1) if kind in (row_round, row_fine, home_round, home_fine) else (3, 2, 1, 0):
            kind(index, peer).start()

    def arrive(kind, index):
        kind(index, 0).wait()
        for peer in PEERS:
            kind(index, peer).wait_recv()

    barrier = pltpu.get_barrier_semaphore()
    for peer in PEERS:
        pl.semaphore_signal(barrier, inc=1, device_id=row_peer(peer), device_id_type=MESH)
        pl.semaphore_signal(barrier, inc=1, device_id=col_peer(peer), device_id_type=MESH)
    pl.semaphore_wait(barrier, 2 * len(PEERS))

    for core, order in enumerate(((2, 3, 1, 0), (3, 2, 1, 0))):

        @pl.when(lax.rem(row, 2) == core)
        def _():
            for peer in order:
                row_fine(0, peer).start()

    @pl.loop(1, PER * EARLY)
    def _(unit):
        start(row_fine, unit)

    start(row_round, 0)

    own_d, far_d = diag.at[chunk(row, S * S)], diag.at[chunk(xor(row, 2), S * S)]
    keep_d = copy(d_ref, own_d, None, d_recv.at[0], None)
    cross_d = copy(d_ref, own_d, d_send.at[1], d_recv.at[1], row_peer(2))
    near_d = copy(d_ref, own_d, d_send.at[2], d_recv.at[2], row_peer(1))
    pass_d = copy(far_d, far_d, d_send.at[3], d_recv.at[3], row_peer(1))
    for start_d in (cross_d, near_d, keep_d):
        start_d.start()

    @pl.loop(1, ROUNDS - EARLY)
    def _(t):
        start(row_round, t)

    factors = [
        pltpu.make_async_copy(a_hbm, a_ref, factor_sem.at[0]),
        pltpu.make_async_copy(b_hbm, b_ref, factor_sem.at[1]),
        pltpu.make_async_copy(c_hbm, c_ref, factor_sem.at[2]),
        pltpu.make_async_copy(a_hbm, a_out, factor_sem.at[3]),
    ]
    for factor in factors:
        factor.start()
    for factor in factors:
        factor.wait()
    b_t[...] = b_ref[...].T
    c_t[...] = c_ref[...].T

    def swapped(matrix, height):
        @pl.loop(0, height // GROUP)
        def _(step):
            lines = [pl.ds(step * GROUP + n, N, stride=height) for n in range(GROUP)]
            side = jnp.concatenate([front[line, :].astype(BF16) for line in lines], axis=1)
            both = dot(matrix[...], side, 1, 0)
            for n, line in enumerate(lines):
                rear[line, :] = both[:, n * N:(n + 1) * N]

    def first_two(view, height):
        @pl.loop(0, 4)
        def _(q):
            block = view[chunk(q)].reshape(S * height, N)
            front[chunk(q, S * height), :] = dot(block, a_ref[...], 1, 1)

        swapped(b_ref, height)

    def fifth(view, height):
        @pl.loop(0, 4)
        def _(q):
            front[chunk(q, S * height), :] = view[chunk(q)].reshape(S * height, N).astype(F32)

        swapped(b_t, height)

    def rounded(view, height):
        @pl.loop(0, 4)
        def _(q):
            view[chunk(q)] = rear[chunk(q, S * height), :].reshape(S, height, N).astype(BF16)

    def fine(here, there, buffer, work, unit):
        arrive(here, unit)
        work(buffer.at[unit], FINE)
        rounded(buffer.at[unit], FINE)
        start(there, unit)

    def whole(here, there, buffer, work, t):
        if here:
            arrive(here, t)

        @pl.loop(0, S // H)
        def _(half):
            view = buffer.at[t, :, chunk(half, H), :]
            work(view, H)
            rounded(view, H)

        start(there, t)

    def middle(t, early):
        if early:
            for n in range(PER):
                arrive(go_fine, PER * t + n)
        else:
            arrive(go_round, t - EARLY)

        @pl.loop(0, S // GROUP)
        def _(step):
            def slab(j):
                return jnp.concatenate([cols[t, c, j] for c in range(4)], axis=0)

            js = [step * GROUP + n for n in range(GROUP)]
            h2 = jnp.concatenate([slab(j) for j in js], axis=1)
            scale = jnp.concatenate([diag_t[j] for j in js], axis=1)
            h3 = (dot(c_ref[...], h2, 1, 0) * scale).astype(BF16)
            h4 = dot(c_t[...], h3, 1, 0).astype(BF16)
            for n, j in enumerate(js):
                for c in range(4):
                    cols[t, c, j] = h4[c * S:(c + 1) * S, n * N:(n + 1) * N]

    def send_back(t, late):
        if late:
            for n in range(PER):
                start(back_fine, PER * (t - ROUNDS + LATE) + n)
        else:
            start(back_round, t)

    first_round = functools.partial(whole, row_round, go_round, tens, first_two)
    fifth_round = functools.partial(whole, None, home_round, rets, fifth)

    pl.loop(0, PER * EARLY)(functools.partial(fine, row_fine, go_fine, fine_in, first_two))
    pl.loop(0, 1)(first_round)
    cross_d.wait_recv()
    pass_d.start()
    keep_d.wait()
    near_d.wait_recv()
    pass_d.wait_recv()

    @pl.loop(0, S)
    def _(j):
        diag_t[j] = diag[pl.ds(j, N, stride=S), :].T

    pl.loop(1, ROUNDS - EARLY)(first_round)
    at_end = lax.rem(col, 3) == 0

    def body(t, early=False, late=False, fifths=True):
        middle(t, early)
        if not fifths:
            send_back(t, late)
            return

        @pl.when(jnp.logical_not(at_end))
        def _():
            send_back(t, late)

        arrive(back_round, t - 1)

        @pl.when(at_end)
        def _():
            send_back(t, late)

        fifth_round(t - 1)

    pl.loop(0, 1)(functools.partial(body, early=True, fifths=False))
    pl.loop(1, ROUNDS - LATE)(body)
    pl.loop(ROUNDS - LATE, ROUNDS)(functools.partial(body, late=True))
    pl.loop(0, PER * LATE)(functools.partial(fine, back_fine, home_fine, fine_out, fifth))

    def finish(kinds, index):
        for kind in kinds:
            if kind in (home_round, home_fine):
                arrive(kind, index)
            for peer in PEERS:
                kind(index, peer).wait_send()

    for sent in (cross_d, near_d, pass_d):
        sent.wait_send()
    pl.loop(0, PER * EARLY)(functools.partial(finish, (row_fine, go_fine)))
    pl.loop(0, ROUNDS - EARLY)(functools.partial(finish, (row_round, go_round)))
    pl.loop(0, ROUNDS - LATE)(functools.partial(finish, (back_round, home_round)))
    pl.loop(0, PER * LATE)(functools.partial(finish, (back_fine, home_fine)))


def last_kernel(h_ref, a_ref, w_ref, out, sem):
    def store(n):
        rows = chunk(n, BLOCK)
        return pltpu.make_async_copy(out.at[rows], w_ref.at[rows], sem.at[n])

    @pl.loop(0, BLOCKS)
    def _(n):
        rows = chunk(n, BLOCK)
        out[rows, :] = dot(h_ref[rows, :], a_ref[...], 1, 0)
        store(n).start()

    @pl.loop(0, BLOCKS)
    def _(n):
        store(n).wait()


def solution(mesh):
    def local_apply(field_u, fac_a, fac_b, fac_c, diag_d):
        batch = field_u.shape[0]
        any_space = pl.BlockSpec(memory_space=pl.ANY)
        vmem = pl.BlockSpec(memory_space=pltpu.VMEM)

        def in_hbm(array):
            return pltpu.with_memory_space_constraint(array, pltpu.HBM)

        operands = (jnp.transpose(field_u, (0, 2, 3, 1)), fac_a, fac_b, fac_c, diag_d.reshape(S * S, N))
        counts = (ROUNDS - EARLY, PER * EARLY) * 2 + (ROUNDS - LATE, PER * LATE) * 2
        pairs = [pltpu.SemaphoreType.DMA((n, 4)) for n in counts for _ in range(2)]
        h5, last_a = pl.pallas_call(
            exchange_kernel,
            out_shape=(pltpu.VMEM((batch, S, S, N), BF16), pltpu.VMEM((N, N), BF16)),
            in_specs=[any_space] * 5,
            out_specs=(any_space, any_space),
            scratch_shapes=[
                pltpu.VMEM((PER * EARLY, N, FINE, N), BF16),
                pltpu.VMEM((ROUNDS - EARLY, N, S, N), BF16),
                pltpu.VMEM((ROUNDS, 4, S, S, N), BF16),
                pltpu.VMEM((ROUNDS - LATE, N, S, N), BF16),
                pltpu.VMEM((PER * LATE, N, FINE, N), BF16),
                pltpu.VMEM((N * H, N), F32),
                pltpu.VMEM((N * H, N), F32),
                pltpu.VMEM((N * S, N), F32),
                pltpu.VMEM((S, N, N), F32),
                pltpu.VMEM((N, N), BF16),
                pltpu.VMEM((N, N), BF16),
                pltpu.VMEM((N, N), BF16),
                pltpu.VMEM((N, N), BF16),
                pltpu.VMEM((N, N), BF16),
                pltpu.SemaphoreType.DMA((4,)),
                pltpu.SemaphoreType.DMA((4,)),
                pltpu.SemaphoreType.DMA((4,)),
                *pairs,
            ],
            compiler_params=pltpu.CompilerParams(
                collective_id=0, has_side_effects=True, vmem_limit_bytes=44 * 2**20
            ),
            name="exchange",
        )(*(in_hbm(operand) for operand in operands))
        w = pl.pallas_call(
            last_kernel,
            out_shape=jax.ShapeDtypeStruct((BLOCKS * BLOCK, N), F32),
            in_specs=[vmem, vmem],
            out_specs=any_space,
            scratch_shapes=[pltpu.VMEM((BLOCKS * BLOCK, N), F32), pltpu.SemaphoreType.DMA((BLOCKS,))],
            compiler_params=pltpu.CompilerParams(vmem_limit_bytes=24 * 2**20),
            name="last",
        )(h5.reshape(BLOCKS * BLOCK, N), last_a)
        return jnp.transpose(w.reshape(batch, S, S, N), (0, 3, 1, 2))

    spec_field = P("fields", None, "row", "col")
    spec_factor = P("fields", None)
    return jax.shard_map(
        local_apply,
        mesh=mesh,
        in_specs=(spec_field, spec_factor, spec_factor, spec_factor, P(("fields", "row"), "col", None)),
        out_specs=spec_field,
        check_vma=False,
    )
```

```python
import functools

import jax
import jax.numpy as jnp
from jax import lax
from jax.experimental import pallas as pl
from jax.experimental.pallas import tpu as pltpu
from jax.sharding import PartitionSpec as P

MESH = pl.DeviceIdType.MESH
N = 128
S = 32
H = 16
FINE = 8
PER = S // FINE
ROUNDS = 8
EARLY = 1
LATE = 1
GROUP = 4
BLOCKS, BLOCK = 16, 2048
F32, BF16 = jnp.float32, jnp.bfloat16
PEERS = (1, 2, 3)


def xor(value, bits):
    if bits == 0:
        return value
    if bits == 1:
        return value + 1 - 2 * lax.rem(value, 2)
    if bits == 2:
        return lax.rem(value + 2, 4)
    return 3 - value


def chunk(index, size=S):
    return pl.ds(pl.multiple_of(index * size, size), size)


def dot(lhs, rhs, lhs_dim, rhs_dim):
    return lax.dot_general(lhs, rhs, (((lhs_dim,), (rhs_dim,)), ((), ())), preferred_element_type=F32)


def exchange_kernel(
    u_ref, a_hbm, b_hbm, c_hbm, d_ref, o_ref, a_out,
    fine_in, tens, cols, rets, fine_out, front, rear, diag, diag_t,
    a_ref, b_ref, c_ref, b_t, c_t, factor_sem, d_send, d_recv, *sems,
):
    row, col = lax.axis_index("row"), lax.axis_index("col")

    def row_peer(dr):
        return {"row": xor(row, dr), "col": col} if dr else None

    def col_peer(dc):
        return {"row": row, "col": xor(col, dc)} if dc else None

    def copy(src, dst, send, recv, peer):
        if not peer:
            return pltpu.make_async_copy(src, dst, recv)
        return pltpu.make_async_remote_copy(
            src_ref=src, dst_ref=dst, send_sem=send, recv_sem=recv, device_id=peer, device_id_type=MESH
        )

    def paired(which, index, offset):
        return sems[2 * which].at[index, offset], sems[2 * which + 1].at[index, offset]

    def row_round(t, dr):
        src = u_ref.at[(t + EARLY) * 4 + xor(row, dr)]
        return copy(src, tens.at[t, chunk(row)], *paired(0, t, dr), row_peer(dr))

    def row_fine(unit, dr):
        t, z = lax.div(unit, PER), lax.rem(unit, PER)
        src = u_ref.at[t * 4 + xor(row, dr), :, chunk(z, FINE), :]
        return copy(src, fine_in.at[unit, chunk(row)], *paired(1, unit, dr), row_peer(dr))

    def go_round(t, dc):
        dst = cols.at[t + EARLY, col]
        return copy(tens.at[t, chunk(xor(col, dc))], dst, *paired(2, t, dc), col_peer(dc))

    def go_fine(unit, dc):
        t, z = lax.div(unit, PER), lax.rem(unit, PER)
        dst = cols.at[t, col, :, chunk(z, FINE), :]
        return copy(fine_in.at[unit, chunk(xor(col, dc))], dst, *paired(3, unit, dc), col_peer(dc))

    def back_round(t, dc):
        src = cols.at[t, xor(col, dc)]
        return copy(src, rets.at[t, chunk(col)], *paired(4, t, dc), col_peer(dc))

    def back_fine(unit, dc):
        t, z = lax.div(unit, PER) + ROUNDS - LATE, lax.rem(unit, PER)
        src = cols.at[t, xor(col, dc), :, chunk(z, FINE), :]
        return copy(src, fine_out.at[unit, chunk(col)], *paired(5, unit, dc), col_peer(dc))

    def home_round(t, dr):
        dst = o_ref.at[t * 4 + row]
        return copy(rets.at[t, chunk(xor(row, dr))], dst, *paired(6, t, dr), row_peer(dr))

    def home_fine(unit, dr):
        t, z = lax.div(unit, PER) + ROUNDS - LATE, lax.rem(unit, PER)
        dst = o_ref.at[t * 4 + row, :, chunk(z, FINE), :]
        return copy(fine_out.at[unit, chunk(xor(row, dr))], dst, *paired(7, unit, dr), row_peer(dr))

    at_end = lax.rem(col, 3) == 0

    def start_back_fine(unit):
        for here, order in ((at_end, (3, 2, 1, 0)), (jnp.logical_not(at_end), (1, 3, 2, 0))):

            @pl.when(here)
            def _():
                for peer in order:
                    back_fine(unit, peer).start()

    def start(kind, index):
        for peer in (0, 3, 2, 1) if kind in (row_round, row_fine, home_round, home_fine) else (3, 2, 1, 0):
            kind(index, peer).start()

    def arrive(kind, index):
        kind(index, 0).wait()
        for peer in PEERS:
            kind(index, peer).wait_recv()

    barrier = pltpu.get_barrier_semaphore()
    for peer in PEERS:
        pl.semaphore_signal(barrier, inc=1, device_id=row_peer(peer), device_id_type=MESH)
        pl.semaphore_signal(barrier, inc=1, device_id=col_peer(peer), device_id_type=MESH)
    pl.semaphore_wait(barrier, 2 * len(PEERS))

    @pl.loop(0, PER * EARLY)
    def _(unit):
        start(row_fine, unit)

    start(row_round, 0)

    own_d, far_d = diag.at[chunk(row, S * S)], diag.at[chunk(xor(row, 2), S * S)]
    keep_d = copy(d_ref, own_d, None, d_recv.at[0], None)
    cross_d = copy(d_ref, own_d, d_send.at[1], d_recv.at[1], row_peer(2))
    near_d = copy(d_ref, own_d, d_send.at[2], d_recv.at[2], row_peer(1))
    pass_d = copy(far_d, far_d, d_send.at[3], d_recv.at[3], row_peer(1))
    for start_d in (cross_d, near_d, keep_d):
        start_d.start()

    @pl.loop(1, ROUNDS - EARLY)
    def _(t):
        start(row_round, t)

    factors = [
        pltpu.make_async_copy(a_hbm, a_ref, factor_sem.at[0]),
        pltpu.make_async_copy(b_hbm, b_ref, factor_sem.at[1]),
        pltpu.make_async_copy(c_hbm, c_ref, factor_sem.at[2]),
        pltpu.make_async_copy(a_hbm, a_out, factor_sem.at[3]),
    ]
    for factor in factors:
        factor.start()
    for factor in factors:
        factor.wait()
    b_t[...] = b_ref[...].T
    c_t[...] = c_ref[...].T

    def swapped(matrix, height):
        @pl.loop(0, height // GROUP)
        def _(step):
            lines = [pl.ds(step * GROUP + n, N, stride=height) for n in range(GROUP)]
            side = jnp.concatenate([front[line, :].astype(BF16) for line in lines], axis=1)
            both = dot(matrix[...], side, 1, 0)
            for n, line in enumerate(lines):
                rear[line, :] = both[:, n * N:(n + 1) * N]

    def first_two(view, height):
        @pl.loop(0, 4)
        def _(q):
            block = view[chunk(q)].reshape(S * height, N)
            front[chunk(q, S * height), :] = dot(block, a_ref[...], 1, 1)

        swapped(b_ref, height)

    def fifth(view, height):
        @pl.loop(0, 4)
        def _(q):
            front[chunk(q, S * height), :] = view[chunk(q)].reshape(S * height, N).astype(F32)

        swapped(b_t, height)

    def rounded(view, height):
        @pl.loop(0, 4)
        def _(q):
            view[chunk(q)] = rear[chunk(q, S * height), :].reshape(S, height, N).astype(BF16)

    def fine(here, there, buffer, work, unit):
        arrive(here, unit)
        work(buffer.at[unit], FINE)
        rounded(buffer.at[unit], FINE)
        start(there, unit)

    def whole(here, there, buffer, work, t):
        if here:
            arrive(here, t)

        @pl.loop(0, S // H)
        def _(half):
            view = buffer.at[t, :, chunk(half, H), :]
            work(view, H)
            rounded(view, H)

        start(there, t)

    def middle(t, early):
        if early:
            for n in range(PER):
                arrive(go_fine, PER * t + n)
        else:
            arrive(go_round, t - EARLY)

        @pl.loop(0, S // GROUP)
        def _(step):
            def slab(j):
                return jnp.concatenate([cols[t, c, j] for c in range(4)], axis=0)

            js = [step * GROUP + n for n in range(GROUP)]
            h2 = jnp.concatenate([slab(j) for j in js], axis=1)
            scale = jnp.concatenate([diag_t[j] for j in js], axis=1)
            h3 = (dot(c_ref[...], h2, 1, 0) * scale).astype(BF16)
            h4 = dot(c_t[...], h3, 1, 0).astype(BF16)
            for n, j in enumerate(js):
                for c in range(4):
                    cols[t, c, j] = h4[c * S:(c + 1) * S, n * N:(n + 1) * N]

    def send_back(t, late):
        if late:
            for n in range(PER):
                start_back_fine(PER * (t - ROUNDS + LATE) + n)
        else:
            start(back_round, t)

    first_round = functools.partial(whole, row_round, go_round, tens, first_two)
    fifth_round = functools.partial(whole, None, home_round, rets, fifth)

    pl.loop(0, PER * EARLY)(functools.partial(fine, row_fine, go_fine, fine_in, first_two))
    pl.loop(0, 1)(first_round)
    cross_d.wait_recv()
    pass_d.start()
    keep_d.wait()
    near_d.wait_recv()
    pass_d.wait_recv()

    @pl.loop(0, S)
    def _(j):
        diag_t[j] = diag[pl.ds(j, N, stride=S), :].T

    pl.loop(1, ROUNDS - EARLY)(first_round)
    def body(t, early=False, late=False, fifths=True):
        middle(t, early)
        if not fifths:
            send_back(t, late)
            return

        @pl.when(jnp.logical_not(at_end))
        def _():
            send_back(t, late)

        arrive(back_round, t - 1)

        @pl.when(at_end)
        def _():
            send_back(t, late)

        fifth_round(t - 1)

    pl.loop(0, 1)(functools.partial(body, early=True, fifths=False))
    pl.loop(1, ROUNDS - LATE)(body)
    pl.loop(ROUNDS - LATE, ROUNDS)(functools.partial(body, late=True))
    pl.loop(0, PER * LATE)(functools.partial(fine, back_fine, home_fine, fine_out, fifth))

    def finish(kinds, index):
        for kind in kinds:
            if kind in (home_round, home_fine):
                arrive(kind, index)
            for peer in PEERS:
                kind(index, peer).wait_send()

    for sent in (cross_d, near_d, pass_d):
        sent.wait_send()
    pl.loop(0, PER * EARLY)(functools.partial(finish, (row_fine, go_fine)))
    pl.loop(0, ROUNDS - EARLY)(functools.partial(finish, (row_round, go_round)))
    pl.loop(0, ROUNDS - LATE)(functools.partial(finish, (back_round, home_round)))
    pl.loop(0, PER * LATE)(functools.partial(finish, (back_fine, home_fine)))


def last_kernel(h_ref, a_ref, w_ref, out, sem):
    def store(n):
        rows = chunk(n, BLOCK)
        return pltpu.make_async_copy(out.at[rows], w_ref.at[rows], sem.at[n])

    @pl.loop(0, BLOCKS)
    def _(n):
        rows = chunk(n, BLOCK)
        out[rows, :] = dot(h_ref[rows, :], a_ref[...], 1, 0)
        store(n).start()

    @pl.loop(0, BLOCKS)
    def _(n):
        store(n).wait()


def solution(mesh):
    def local_apply(field_u, fac_a, fac_b, fac_c, diag_d):
        batch = field_u.shape[0]
        any_space = pl.BlockSpec(memory_space=pl.ANY)
        vmem = pl.BlockSpec(memory_space=pltpu.VMEM)

        def in_hbm(array):
            return pltpu.with_memory_space_constraint(array, pltpu.HBM)

        operands = (jnp.transpose(field_u, (0, 2, 3, 1)), fac_a, fac_b, fac_c, diag_d.reshape(S * S, N))
        counts = (ROUNDS - EARLY, PER * EARLY) * 2 + (ROUNDS - LATE, PER * LATE) * 2
        pairs = [pltpu.SemaphoreType.DMA((n, 4)) for n in counts for _ in range(2)]
        h5, last_a = pl.pallas_call(
            exchange_kernel,
            out_shape=(pltpu.VMEM((batch, S, S, N), BF16), pltpu.VMEM((N, N), BF16)),
            in_specs=[any_space] * 5,
            out_specs=(any_space, any_space),
            scratch_shapes=[
                pltpu.VMEM((PER * EARLY, N, FINE, N), BF16),
                pltpu.VMEM((ROUNDS - EARLY, N, S, N), BF16),
                pltpu.VMEM((ROUNDS, 4, S, S, N), BF16),
                pltpu.VMEM((ROUNDS - LATE, N, S, N), BF16),
                pltpu.VMEM((PER * LATE, N, FINE, N), BF16),
                pltpu.VMEM((N * H, N), F32),
                pltpu.VMEM((N * H, N), F32),
                pltpu.VMEM((N * S, N), F32),
                pltpu.VMEM((S, N, N), F32),
                pltpu.VMEM((N, N), BF16),
                pltpu.VMEM((N, N), BF16),
                pltpu.VMEM((N, N), BF16),
                pltpu.VMEM((N, N), BF16),
                pltpu.VMEM((N, N), BF16),
                pltpu.SemaphoreType.DMA((4,)),
                pltpu.SemaphoreType.DMA((4,)),
                pltpu.SemaphoreType.DMA((4,)),
                *pairs,
            ],
            compiler_params=pltpu.CompilerParams(
                collective_id=0, has_side_effects=True, vmem_limit_bytes=44 * 2**20
            ),
            name="exchange",
        )(*(in_hbm(operand) for operand in operands))
        w = pl.pallas_call(
            last_kernel,
            out_shape=jax.ShapeDtypeStruct((BLOCKS * BLOCK, N), F32),
            in_specs=[vmem, vmem],
            out_specs=any_space,
            scratch_shapes=[pltpu.VMEM((BLOCKS * BLOCK, N), F32), pltpu.SemaphoreType.DMA((BLOCKS,))],
            compiler_params=pltpu.CompilerParams(vmem_limit_bytes=24 * 2**20),
            name="last",
        )(h5.reshape(BLOCKS * BLOCK, N), last_a)
        return jnp.transpose(w.reshape(batch, S, S, N), (0, 3, 1, 2))

    spec_field = P("fields", None, "row", "col")
    spec_factor = P("fields", None)
    return jax.shard_map(
        local_apply,
        mesh=mesh,
        in_specs=(spec_field, spec_factor, spec_factor, spec_factor, P(("fields", "row"), "col", None)),
        out_specs=spec_field,
        check_vma=False,
    )
```
